32 devices in a mesh: first: 4 (over y, x), second: 8 (over z, core).
Axes of the slice: x: 2, y: 2, z: 4, core: 2. Of those that a mesh axis runs over, the one named last changes fastest.
Arguments:
- pair_state: bfloat16 [96, 96, 128], P('first', 'second'), may hold values from -6 to 6
- in_gain: float32 [128], replicated, may hold values from 0.25 to 1.75
- left_weight: bfloat16 [128, 128], replicated, may hold values from -0.5 to 0.5
- right_weight: bfloat16 [128, 128], replicated, may hold values from -0.5 to 0.5
- mid_gain: float32 [128], replicated, may hold values from 0.25 to 1.75
- out_weight: bfloat16 [128, 128], replicated, may hold values from -0.5 to 0.5
- out_gate: bfloat16 [128, 128], replicated, may hold values from -0.5 to 0.5
Outputs:
- triangle_out: bfloat16 [96, 96, 128], P('first', 'second')
The draws below stay inside these ranges and needn't reach their ends.
All inputs are finite; a program needn't handle non-finite values.
Results may differ from the reference program's by a relative error of at most 0.015.
Values may be sent and summed in bfloat16 or wider, within the bound.
A program may use at most 64 MiB of HBM per device.

```python
import jax
import jax.numpy as jnp
from jax import lax

RESIDUES = 96
PAIR_WIDTH = 128
MIX_WIDTH = 128


def shard_levels(own_key, extent, cuts, smallest, largest):
    def one(axis_at, parts):
        draws = jax.random.uniform(jax.random.fold_in(jax.random.fold_in(own_key, 6), axis_at), (parts,), jnp.float32, smallest / len(cuts), largest / len(cuts))
        return jnp.repeat(jnp.exp(draws), extent[axis_at] // parts).reshape((-1,) + (1,) * (len(extent) - axis_at - 1))

    factor_of = one(*cuts[0])
    for cut in cuts[1:]:
        factor_of = factor_of * one(*cut)
    return factor_of


def scatter_about(key, extent, scale, bound, split=(), kind=jnp.bfloat16):
    gain = shard_levels(key, extent, split, -0.22, 0.18) if split else 1.0
    values = jax.random.normal(key, extent, jnp.float32) * scale * gain
    return jnp.minimum(jnp.maximum(values, -bound), bound).astype(kind)


def setup_inputs(seed: int = 0) -> dict:
    arg_keys = jax.random.split(jax.random.key(seed), 8)
    return {
        "pair_state": scatter_about(arg_keys[0], (RESIDUES, RESIDUES, PAIR_WIDTH), 1.0, 6.0, ((0, 4), (1, 8))),
        "in_gain": jnp.clip(1.0 + 0.15 * jax.random.normal(arg_keys[1], (PAIR_WIDTH,), jnp.float32), 0.25, 1.75),
        "left_weight": scatter_about(arg_keys[2], (PAIR_WIDTH, MIX_WIDTH), PAIR_WIDTH ** -0.5, 0.5),
        "right_weight": scatter_about(arg_keys[3], (PAIR_WIDTH, MIX_WIDTH), PAIR_WIDTH ** -0.5, 0.5),
        "mid_gain": jnp.clip(1.0 + 0.15 * jax.random.normal(arg_keys[4], (MIX_WIDTH,), jnp.float32), 0.25, 1.75),
        "out_weight": scatter_about(arg_keys[5], (MIX_WIDTH, PAIR_WIDTH), MIX_WIDTH ** -0.5, 0.5),
        "out_gate": scatter_about(arg_keys[6], (PAIR_WIDTH, PAIR_WIDTH), PAIR_WIDTH ** -0.5, 0.5),
    }


def unit_channels(values, channel_gain):
    centred = values - lax.optimization_barrier(jnp.mean(values, axis=-1, keepdims=True))
    return centred * lax.rsqrt(lax.optimization_barrier(jnp.mean(centred * centred, axis=-1, keepdims=True)) + 1e-05) * channel_gain

def make_factors(pair_in, in_gain, left_weight, right_weight):
    ready = unit_channels(pair_in.astype(jnp.float32), in_gain).astype(jnp.bfloat16)
    ready = lax.optimization_barrier(ready)
    left = jnp.einsum('ijc,cd->ijd', ready.astype(jnp.float32), left_weight.astype(jnp.float32))
    right = jnp.einsum('ijc,cd->ijd', ready.astype(jnp.float32), right_weight.astype(jnp.float32))
    return (ready, left.astype(jnp.bfloat16), right.astype(jnp.bfloat16))

def finish_pair(mixed, ready, mid_gain, out_weight, out_gate):
    scaled = unit_channels(mixed.astype(jnp.float32), mid_gain).astype(jnp.bfloat16)
    scaled = lax.optimization_barrier(scaled)
    gate = jax.nn.sigmoid(jnp.einsum('ijc,cd->ijd', ready.astype(jnp.float32), out_gate.astype(jnp.float32)))
    return (jnp.einsum('ijd,dc->ijc', scaled.astype(jnp.float32), out_weight.astype(jnp.float32)) * gate).astype(jnp.bfloat16)

def reference(pair_state, in_gain, left_weight, right_weight, mid_gain, out_weight, out_gate):
    ready, left, right = make_factors(pair_state, in_gain, left_weight, right_weight)
    left, right = lax.optimization_barrier((left, right))

    def one_channel(pair_of):
        return (jnp.dot(pair_of[0], pair_of[1].T, preferred_element_type=jnp.float32) * RESIDUES ** (-0.5)).astype(jnp.bfloat16)
    mixed = jnp.moveaxis(lax.map(one_channel, (jnp.moveaxis(left, -1, 0), jnp.moveaxis(right, -1, 0))), 0, -1)
    mixed = lax.optimization_barrier(mixed)
    return finish_pair(mixed, ready, mid_gain, out_weight, out_gate)
```

```python
import functools

import jax
import jax.numpy as jnp
from jax import lax
from jax.experimental import pallas as pl
from jax.experimental.pallas import tpu as pltpu
from jax.sharding import PartitionSpec as P

MESH = pl.DeviceIdType.MESH
F32 = jnp.float32
BF16 = jnp.bfloat16
CORES = 2


def unit_channels(values, channel_gain):
    centred = values - jnp.mean(values, axis=-1, keepdims=True)
    return (
        centred
        * lax.rsqrt(jnp.mean(centred * centred, axis=-1, keepdims=True) + 1e-05)
        * channel_gain
    )


def bit_xor(left, right, count):
    total, bit = 0, 1
    while bit < count:
        total = total + (left // bit % 2 + right // bit % 2) % 2 * bit
        bit *= 2
    return total


def triangle_kernel(
    groups, count,
    x_ref, in_gain, left_weight, right_weight, mid_gain, out_weight, out_gate, out_ref,
    spread, left_send, left_recv, right_send, right_recv, right_rows, left_f, right_f,
    part_send, part_recv, own_part, gate,
    left_sems, right_send_sems, right_recv_sems, part_send_sems, part_recv_sems,
):
    rows, cols, width = x_ref.shape
    pitch = spread.shape[0] // rows
    half = rows // CORES
    pairs = rows * cols
    a = lax.axis_index("first")
    b = lax.axis_index("second")
    z, c = b // CORES, b % CORES
    other = 1 - c

    def core_at(first, layer, core):
        return {"first": first, "second": layer * CORES + core}

    barrier = pltpu.get_barrier_semaphore()
    peers = [core_at(a, z, other)]
    for s in range(1, groups):
        peers += [core_at(bit_xor(a, s, groups), z, c), core_at(bit_xor(a, s, groups), z, other)]
        peers.append(core_at(a, bit_xor(z, s, groups), c))
    for peer in peers:
        pl.semaphore_signal(barrier, inc=1, device_id=peer, device_id_type=MESH)

    for i in range(rows):
        spread[i * pitch : i * pitch + cols, :] = x_ref[i].astype(F32)
    values = jnp.concatenate([spread[pl.ds(k, rows, stride=pitch), :] for k in range(cols)], axis=0)
    ready = unit_channels(values, in_gain[...].reshape(1, width)).astype(BF16)

    right_rows[...] = jnp.dot(ready, right_weight[...], preferred_element_type=F32)
    for p in range(CORES):
        for k in range(cols):
            right_f[p, k * half : (k + 1) * half, :] = right_rows[
                k * rows + p * half : k * rows + (p + 1) * half, :
            ]
    for p in range(CORES):
        right_send[p] = right_f[p].astype(BF16)

    pl.semaphore_wait(barrier, len(peers))

    right_copies = {}
    for s in range(groups):
        for r in range(CORES):
            if s == 0 and r == 0:
                continue
            core = c if r == 0 else other
            copy = pltpu.make_async_remote_copy(
                src_ref=right_send.at[core],
                dst_ref=right_recv.at[s, r],
                send_sem=right_send_sems.at[s, r],
                recv_sem=right_recv_sems.at[s, r],
                device_id=core_at(bit_xor(a, s, groups), z, core),
                device_id_type=MESH,
            )
            copy.start()
            right_copies[s, r] = copy

    left = jnp.dot(ready, left_weight[...], preferred_element_type=F32).astype(BF16)
    left_send[...] = left
    left_f[0] = left.astype(F32)
    left_copy = pltpu.make_async_remote_copy(
        src_ref=left_send,
        dst_ref=left_recv,
        send_sem=left_sems.at[0],
        recv_sem=left_sems.at[1],
        device_id=core_at(a, z, other),
        device_id_type=MESH,
    )
    left_copy.start()

    gate[...] = jax.nn.sigmoid(jnp.dot(ready, out_gate[...], preferred_element_type=F32))

    left_copy.wait_recv()
    left_f[1] = left_recv[...].astype(F32)

    part_copies = []
    for s in range(groups):
        if s == 0:
            right_f[0] = right_send[c].astype(F32)
        else:
            right_copies[s, 0].wait_recv()
            right_f[0] = right_recv[s, 0].astype(F32)
        right_copies[s, 1].wait_recv()
        right_f[1] = right_recv[s, 1].astype(F32)

        def step(k, sums):
            sums = list(sums)
            for r in range(CORES):
                line = left_f[r, pl.ds(pl.multiple_of(k * rows, 8), rows), :]
                for j in range(half):
                    sums[j] = sums[j] + line * right_f[r, pl.ds(k * half + j, 1), :]
            return tuple(sums)

        sums = lax.fori_loop(
            0, cols, step, tuple(jnp.zeros((rows, width), F32) for _ in range(half))
        )
        part = jnp.concatenate(sums, axis=0)
        part_send[s] = part.astype(BF16)
        layer = bit_xor(a, s, groups)
        turn = bit_xor(layer, z, groups)
        copy = pltpu.make_async_remote_copy(
            src_ref=part_send.at[s],
            dst_ref=part_recv.at[turn],
            send_sem=part_send_sems.at[s],
            recv_sem=part_recv_sems.at[turn],
            device_id=core_at(a, layer, c),
            device_id_type=MESH,
        )

        @pl.when(turn != 0)
        def _():
            copy.start()

        @pl.when(turn == 0)
        def _():
            own_part[...] = part

        part_copies.append((turn, copy))

    total = own_part[...]
    for t in range(1, groups):
        pltpu.make_async_remote_copy(
            src_ref=part_send.at[0],
            dst_ref=part_recv.at[t],
            send_sem=part_send_sems.at[0],
            recv_sem=part_recv_sems.at[t],
            device_id=core_at(a, bit_xor(z, t, groups), c),
            device_id_type=MESH,
        ).wait_recv()
        total = total + part_recv[t].astype(F32)

    mixed = (total * count ** (-0.5)).astype(BF16).astype(F32)
    scaled = unit_channels(mixed, mid_gain[...].reshape(1, width)).astype(BF16)
    right_rows[...] = (
        jnp.dot(scaled, out_weight[...], preferred_element_type=F32) * gate[...]
    )
    for i in range(rows):
        out_ref[i] = right_rows[pl.ds(i, cols, stride=rows), :].astype(BF16)

    left_copy.wait_send()
    for copy in right_copies.values():
        copy.wait_send()
    for turn, copy in part_copies:

        @pl.when(turn != 0)
        def _(copy=copy):
            copy.wait_send()


def by_kernel(pair_state, in_gain, left_weight, right_weight, mid_gain, out_weight, out_gate):
    rows, cols, width = pair_state.shape
    groups = lax.axis_size("first")
    count = cols * lax.axis_size("second")
    pairs = rows * cols
    half = pairs // CORES
    pitch = -(-cols // 8) * 8
    vmem = pl.BlockSpec(memory_space=pltpu.VMEM)
    return pl.pallas_call(
        functools.partial(triangle_kernel, groups, count),
        out_shape=jax.ShapeDtypeStruct((rows, cols, width), BF16),
        in_specs=[vmem] * 7,
        out_specs=vmem,
        scratch_shapes=[
            pltpu.VMEM((rows * pitch, width), F32),
            pltpu.VMEM((pairs, width), BF16),
            pltpu.VMEM((pairs, width), BF16),
            pltpu.VMEM((CORES, half, width), BF16),
            pltpu.VMEM((groups, CORES, half, width), BF16),
            pltpu.VMEM((pairs, width), F32),
            pltpu.VMEM((CORES, pairs, width), F32),
            pltpu.VMEM((CORES, half, width), F32),
            pltpu.VMEM((groups, pairs, width), BF16),
            pltpu.VMEM((groups, pairs, width), BF16),
            pltpu.VMEM((pairs, width), F32),
            pltpu.VMEM((pairs, width), F32),
            pltpu.SemaphoreType.DMA((2,)),
            pltpu.SemaphoreType.DMA((groups, CORES)),
            pltpu.SemaphoreType.DMA((groups, CORES)),
            pltpu.SemaphoreType.DMA((groups,)),
            pltpu.SemaphoreType.DMA((groups,)),
        ],
        compiler_params=pltpu.CompilerParams(collective_id=0, has_side_effects=True),
    )(pair_state, in_gain, left_weight, right_weight, mid_gain, out_weight, out_gate)


def make_factors(pair_in, in_gain, left_weight, right_weight):
    ready = unit_channels(pair_in.astype(jnp.float32), in_gain).astype(jnp.bfloat16)
    ready = lax.optimization_barrier(ready)
    left = jnp.einsum("ijc,cd->ijd", ready, left_weight, preferred_element_type=jnp.float32)
    right = jnp.einsum("ijc,cd->ijd", ready, right_weight, preferred_element_type=jnp.float32)
    return (ready, left.astype(jnp.bfloat16), right.astype(jnp.bfloat16))


def finish_pair(mixed, ready, mid_gain, out_weight, out_gate):
    scaled = unit_channels(mixed.astype(jnp.float32), mid_gain).astype(jnp.bfloat16)
    scaled = lax.optimization_barrier(scaled)
    gate = jax.nn.sigmoid(
        jnp.einsum("ijc,cd->ijd", ready, out_gate, preferred_element_type=jnp.float32)
    )
    return (
        jnp.einsum("ijd,dc->ijc", scaled, out_weight, preferred_element_type=jnp.float32) * gate
    ).astype(jnp.bfloat16)


def by_collectives(pair_state, in_gain, left_weight, right_weight, mid_gain, out_weight, out_gate):
    ready, left, right = make_factors(pair_state, in_gain, left_weight, right_weight)
    count = pair_state.shape[1] * lax.axis_size("second")
    left_lines, right_lines = (
        lax.all_to_all(left, "second", split_axis=2, concat_axis=1, tiled=True),
        lax.all_to_all(right, "second", split_axis=2, concat_axis=1, tiled=True),
    )

    def meet(piece):
        return jnp.einsum("ikd,jkd->ijd", left_lines, piece, preferred_element_type=jnp.float32)

    strip = meet(lax.all_gather(right_lines, "first", axis=0, tiled=True))
    strip = (strip * count ** (-0.5)).astype(jnp.bfloat16)
    mixed = lax.all_to_all(strip, "second", split_axis=1, concat_axis=2, tiled=True)
    return finish_pair(mixed, ready, mid_gain, out_weight, out_gate)


def per_device(pair_state, *rest):
    groups, parts = lax.axis_size("first"), lax.axis_size("second")
    rows, cols, width = pair_state.shape
    fits = (
        parts == CORES * groups
        and groups & (groups - 1) == 0
        and rows == CORES * cols
        and rows % 8 == 0
        and rows * cols % 32 == 0
        and rows // 8 * cols <= 48
    )
    return (by_kernel if fits else by_collectives)(pair_state, *rest)


def solution(mesh):
    in_specs = (P("first", "second", None), P(), P(), P(), P(), P(), P())
    out_specs = P("first", "second", None)
    return jax.shard_map(
        per_device, mesh=mesh, in_specs=in_specs, out_specs=out_specs, check_vma=False
    )
```

```python
import functools

import jax
import jax.numpy as jnp
from jax import lax
from jax.experimental import pallas as pl
from jax.experimental.pallas import tpu as pltpu
from jax.sharding import PartitionSpec as P

MESH = pl.DeviceIdType.MESH
F32 = jnp.float32
BF16 = jnp.bfloat16
CORES = 2


def unit_channels(values, channel_gain):
    centred = values - jnp.mean(values, axis=-1, keepdims=True)
    return (
        centred
        * lax.rsqrt(jnp.mean(centred * centred, axis=-1, keepdims=True) + 1e-05)
        * channel_gain
    )


def bit_xor(left, right, count):
    total, bit = 0, 1
    while bit < count:
        total = total + (left // bit % 2 + right // bit % 2) % 2 * bit
        bit *= 2
    return total


def triangle_kernel(
    groups, count,
    x_ref, in_gain, left_weight, right_weight, mid_gain, out_weight, out_gate, out_ref,
    left_send, left_recv, right_send, right_recv, right_rows, left_f, right_f,
    part_send, part_recv, own_part, gate,
    left_sems, right_send_sems, right_recv_sems, part_send_sems, part_recv_sems,
):
    cols, rows, width = x_ref.shape
    half = rows // CORES
    pairs = rows * cols
    a = lax.axis_index("first")
    b = lax.axis_index("second")
    z, c = b // CORES, b % CORES
    other = 1 - c

    def core_at(first, layer, core):
        return {"first": first, "second": layer * CORES + core}

    barrier = pltpu.get_barrier_semaphore()
    peers = [core_at(a, z, other)]
    for s in range(1, groups):
        peers += [core_at(bit_xor(a, s, groups), z, c), core_at(bit_xor(a, s, groups), z, other)]
        peers.append(core_at(a, bit_xor(z, s, groups), c))
    for peer in peers:
        pl.semaphore_signal(barrier, inc=1, device_id=peer, device_id_type=MESH)

    values = x_ref[...].astype(F32).reshape(pairs, width)
    ready = unit_channels(values, in_gain[...].reshape(1, width)).astype(BF16)

    right_rows[...] = jnp.dot(ready, right_weight[...], preferred_element_type=F32)
    for p in range(CORES):
        for k in range(cols):
            right_f[p, k * half : (k + 1) * half, :] = right_rows[
                k * rows + p * half : k * rows + (p + 1) * half, :
            ]
    for p in range(CORES):
        right_send[p] = right_f[p].astype(BF16)

    pl.semaphore_wait(barrier, len(peers))

    right_copies = {}
    for s in range(groups):
        for r in range(CORES):
            if s == 0 and r == 0:
                continue
            core = c if r == 0 else other
            copy = pltpu.make_async_remote_copy(
                src_ref=right_send.at[core],
                dst_ref=right_recv.at[s, r],
                send_sem=right_send_sems.at[s, r],
                recv_sem=right_recv_sems.at[s, r],
                device_id=core_at(bit_xor(a, s, groups), z, core),
                device_id_type=MESH,
            )
            copy.start()
            right_copies[s, r] = copy

    left = jnp.dot(ready, left_weight[...], preferred_element_type=F32).astype(BF16)
    left_send[...] = left
    left_f[0] = left.astype(F32)
    left_copy = pltpu.make_async_remote_copy(
        src_ref=left_send,
        dst_ref=left_recv,
        send_sem=left_sems.at[0],
        recv_sem=left_sems.at[1],
        device_id=core_at(a, z, other),
        device_id_type=MESH,
    )
    left_copy.start()

    gate[...] = jax.nn.sigmoid(jnp.dot(ready, out_gate[...], preferred_element_type=F32))

    left_copy.wait_recv()
    left_f[1] = left_recv[...].astype(F32)

    part_copies = []
    for s in range(groups):
        if s == 0:
            right_f[0] = right_send[c].astype(F32)
        else:
            right_copies[s, 0].wait_recv()
            right_f[0] = right_recv[s, 0].astype(F32)
        right_copies[s, 1].wait_recv()
        right_f[1] = right_recv[s, 1].astype(F32)

        def step(k, sums):
            sums = list(sums)
            for r in range(CORES):
                line = left_f[r, pl.ds(pl.multiple_of(k * rows, 8), rows), :]
                for j in range(half):
                    sums[j] = sums[j] + line * right_f[r, pl.ds(k * half + j, 1), :]
            return tuple(sums)

        sums = lax.fori_loop(
            0, cols, step, tuple(jnp.zeros((rows, width), F32) for _ in range(half))
        )
        part = jnp.concatenate(sums, axis=0)
        part_send[s] = part.astype(BF16)
        layer = bit_xor(a, s, groups)
        turn = bit_xor(layer, z, groups)
        copy = pltpu.make_async_remote_copy(
            src_ref=part_send.at[s],
            dst_ref=part_recv.at[turn],
            send_sem=part_send_sems.at[s],
            recv_sem=part_recv_sems.at[turn],
            device_id=core_at(a, layer, c),
            device_id_type=MESH,
        )

        @pl.when(turn != 0)
        def _():
            copy.start()

        @pl.when(turn == 0)
        def _():
            own_part[...] = part

        part_copies.append((turn, copy))

    total = own_part[...]
    for t in range(1, groups):
        pltpu.make_async_remote_copy(
            src_ref=part_send.at[0],
            dst_ref=part_recv.at[t],
            send_sem=part_send_sems.at[0],
            recv_sem=part_recv_sems.at[t],
            device_id=core_at(a, bit_xor(z, t, groups), c),
            device_id_type=MESH,
        ).wait_recv()
        total = total + part_recv[t].astype(F32)

    mixed = (total * count ** (-0.5)).astype(BF16).astype(F32)
    scaled = unit_channels(mixed, mid_gain[...].reshape(1, width)).astype(BF16)
    result = jnp.dot(scaled, out_weight[...], preferred_element_type=F32) * gate[...]
    out_ref[...] = result.reshape(cols, rows, width).astype(BF16)

    left_copy.wait_send()
    for copy in right_copies.values():
        copy.wait_send()
    for turn, copy in part_copies:

        @pl.when(turn != 0)
        def _(copy=copy):
            copy.wait_send()


def by_kernel(pair_state, in_gain, left_weight, right_weight, mid_gain, out_weight, out_gate):
    rows, cols, width = pair_state.shape
    groups = lax.axis_size("first")
    count = cols * lax.axis_size("second")
    pairs = rows * cols
    half = pairs // CORES
    vmem = pl.BlockSpec(memory_space=pltpu.VMEM)
    changed = pl.pallas_call(
        functools.partial(triangle_kernel, groups, count),
        out_shape=jax.ShapeDtypeStruct((cols, rows, width), BF16),
        in_specs=[vmem] * 7,
        out_specs=vmem,
        scratch_shapes=[
            pltpu.VMEM((pairs, width), BF16),
            pltpu.VMEM((pairs, width), BF16),
            pltpu.VMEM((CORES, half, width), BF16),
            pltpu.VMEM((groups, CORES, half, width), BF16),
            pltpu.VMEM((pairs, width), F32),
            pltpu.VMEM((CORES, pairs, width), F32),
            pltpu.VMEM((CORES, half, width), F32),
            pltpu.VMEM((groups, pairs, width), BF16),
            pltpu.VMEM((groups, pairs, width), BF16),
            pltpu.VMEM((pairs, width), F32),
            pltpu.VMEM((pairs, width), F32),
            pltpu.SemaphoreType.DMA((2,)),
            pltpu.SemaphoreType.DMA((groups, CORES)),
            pltpu.SemaphoreType.DMA((groups, CORES)),
            pltpu.SemaphoreType.DMA((groups,)),
            pltpu.SemaphoreType.DMA((groups,)),
        ],
        compiler_params=pltpu.CompilerParams(collective_id=0, has_side_effects=True),
    )(
        jnp.swapaxes(pair_state, 0, 1),
        in_gain, left_weight, right_weight, mid_gain, out_weight, out_gate,
    )
    return jnp.swapaxes(changed, 0, 1)


def make_factors(pair_in, in_gain, left_weight, right_weight):
    ready = unit_channels(pair_in.astype(jnp.float32), in_gain).astype(jnp.bfloat16)
    ready = lax.optimization_barrier(ready)
    left = jnp.einsum("ijc,cd->ijd", ready, left_weight, preferred_element_type=jnp.float32)
    right = jnp.einsum("ijc,cd->ijd", ready, right_weight, preferred_element_type=jnp.float32)
    return (ready, left.astype(jnp.bfloat16), right.astype(jnp.bfloat16))


def finish_pair(mixed, ready, mid_gain, out_weight, out_gate):
    scaled = unit_channels(mixed.astype(jnp.float32), mid_gain).astype(jnp.bfloat16)
    scaled = lax.optimization_barrier(scaled)
    gate = jax.nn.sigmoid(
        jnp.einsum("ijc,cd->ijd", ready, out_gate, preferred_element_type=jnp.float32)
    )
    return (
        jnp.einsum("ijd,dc->ijc", scaled, out_weight, preferred_element_type=jnp.float32) * gate
    ).astype(jnp.bfloat16)


def by_collectives(pair_state, in_gain, left_weight, right_weight, mid_gain, out_weight, out_gate):
    ready, left, right = make_factors(pair_state, in_gain, left_weight, right_weight)
    count = pair_state.shape[1] * lax.axis_size("second")
    left_lines, right_lines = (
        lax.all_to_all(left, "second", split_axis=2, concat_axis=1, tiled=True),
        lax.all_to_all(right, "second", split_axis=2, concat_axis=1, tiled=True),
    )

    def meet(piece):
        return jnp.einsum("ikd,jkd->ijd", left_lines, piece, preferred_element_type=jnp.float32)

    strip = meet(lax.all_gather(right_lines, "first", axis=0, tiled=True))
    strip = (strip * count ** (-0.5)).astype(jnp.bfloat16)
    mixed = lax.all_to_all(strip, "second", split_axis=1, concat_axis=2, tiled=True)
    return finish_pair(mixed, ready, mid_gain, out_weight, out_gate)


def per_device(pair_state, *rest):
    groups, parts = lax.axis_size("first"), lax.axis_size("second")
    rows, cols, width = pair_state.shape
    fits = (
        parts == CORES * groups
        and groups & (groups - 1) == 0
        and rows == CORES * cols
        and rows % 8 == 0
        and rows * cols % 32 == 0
        and rows // 8 * cols <= 48
    )
    return (by_kernel if fits else by_collectives)(pair_state, *rest)


def solution(mesh):
    in_specs = (P("first", "second", None), P(), P(), P(), P(), P(), P())
    out_specs = P("first", "second", None)
    return jax.shard_map(
        per_device, mesh=mesh, in_specs=in_specs, out_specs=out_specs, check_vma=False
    )
```

```python
import functools

import jax
import jax.numpy as jnp
from jax import lax
from jax.experimental import pallas as pl
from jax.experimental.pallas import tpu as pltpu
from jax.sharding import PartitionSpec as P

MESH = pl.DeviceIdType.MESH
F32 = jnp.float32
BF16 = jnp.bfloat16
CORES = 2


def unit_channels(values, channel_gain):
    centred = values - jnp.mean(values, axis=-1, keepdims=True)
    return (
        centred
        * lax.rsqrt(jnp.mean(centred * centred, axis=-1, keepdims=True) + 1e-05)
        * channel_gain
    )


def bit_xor(left, right, count):
    total, bit = 0, 1
    while bit < count:
        total = total + (left // bit % 2 + right // bit % 2) % 2 * bit
        bit *= 2
    return total


def triangle_kernel(
    groups, count,
    x_hbm, in_gain_hbm, left_weight_hbm, right_weight_hbm, mid_gain_hbm, out_weight_hbm,
    out_gate_hbm, out_ref,
    x_ref, in_gain, left_weight, right_weight, mid_gain, out_weight, out_gate, fetch_sems,
    left_send, left_recv, right_send, right_recv, right_rows, left_f, right_f,
    part_send, part_recv, own_part, gate,
    left_sems, right_send_sems, right_recv_sems, part_send_sems, part_recv_sems,
):
    cols, rows, width = x_ref.shape
    half = rows // CORES
    pairs = rows * cols
    a = lax.axis_index("first")
    b = lax.axis_index("second")
    z, c = b // CORES, b % CORES
    other = 1 - c

    def core_at(first, layer, core):
        return {"first": first, "second": layer * CORES + core}

    barrier = pltpu.get_barrier_semaphore()
    peers = [core_at(a, z, other)]
    for s in range(1, groups):
        peers += [core_at(bit_xor(a, s, groups), z, c), core_at(bit_xor(a, s, groups), z, other)]
        peers.append(core_at(a, bit_xor(z, s, groups), c))
    for peer in peers:
        pl.semaphore_signal(barrier, inc=1, device_id=peer, device_id_type=MESH)

    fetches = [
        pltpu.make_async_copy(src, dst, fetch_sems.at[n])
        for n, (src, dst) in enumerate([
            (x_hbm, x_ref), (in_gain_hbm, in_gain), (right_weight_hbm, right_weight),
            (left_weight_hbm, left_weight), (out_gate_hbm, out_gate),
            (mid_gain_hbm, mid_gain), (out_weight_hbm, out_weight),
        ])
    ]
    for fetch in fetches:
        fetch.start()
    for fetch in fetches:
        fetch.wait()

    values = x_ref[...].astype(F32).reshape(pairs, width)
    ready = unit_channels(values, in_gain[...].reshape(1, width)).astype(BF16)

    right_rows[...] = jnp.dot(ready, right_weight[...], preferred_element_type=F32)
    for p in range(CORES):
        for k in range(cols):
            right_f[p, k * half : (k + 1) * half, :] = right_rows[
                k * rows + p * half : k * rows + (p + 1) * half, :
            ]
    for p in range(CORES):
        right_send[p] = right_f[p].astype(BF16)

    pl.semaphore_wait(barrier, len(peers))

    inner = (a % (groups - 1) + groups - 2) // (groups - 1)
    turns = [0] + [
        inner * s + (1 - inner) * ((groups - 1) if s == 1 else s - 1)
        for s in range(1, groups)
    ]

    def right_copy(s, r):
        core = c if r == 0 else other
        return pltpu.make_async_remote_copy(
            src_ref=right_send.at[core],
            dst_ref=right_recv.at[s, r],
            send_sem=right_send_sems.at[s, r],
            recv_sem=right_recv_sems.at[s, r],
            device_id=core_at(bit_xor(a, s, groups), z, core),
            device_id_type=MESH,
        )

    right_copies = [
        right_copy(s, r) for n, s in enumerate(turns) for r in range(CORES) if (n, r) != (0, 0)
    ]
    for copy in right_copies:
        copy.start()

    left = jnp.dot(ready, left_weight[...], preferred_element_type=F32).astype(BF16)
    left_send[...] = left
    left_f[0] = left.astype(F32)
    left_copy = pltpu.make_async_remote_copy(
        src_ref=left_send,
        dst_ref=left_recv,
        send_sem=left_sems.at[0],
        recv_sem=left_sems.at[1],
        device_id=core_at(a, z, other),
        device_id_type=MESH,
    )
    left_copy.start()

    gate[...] = jax.nn.sigmoid(jnp.dot(ready, out_gate[...], preferred_element_type=F32))

    left_copy.wait_recv()
    left_f[1] = left_recv[...].astype(F32)

    part_copies = []
    for n, s in enumerate(turns):
        if n == 0:
            right_f[0] = right_send[c].astype(F32)
        else:
            right_copy(s, 0).wait_recv()
            right_f[0] = right_recv[s, 0].astype(F32)
        right_copy(s, 1).wait_recv()
        right_f[1] = right_recv[s, 1].astype(F32)

        def step(k, sums):
            sums = list(sums)
            for r in range(CORES):
                line = left_f[r, pl.ds(pl.multiple_of(k * rows, 8), rows), :]
                for j in range(half):
                    sums[j] = sums[j] + line * right_f[r, pl.ds(k * half + j, 1), :]
            return tuple(sums)

        sums = lax.fori_loop(
            0, cols, step, tuple(jnp.zeros((rows, width), F32) for _ in range(half))
        )
        part = jnp.concatenate(sums, axis=0)
        part_send[n] = part.astype(BF16)
        layer = bit_xor(a, s, groups)
        turn = bit_xor(layer, z, groups)
        copy = pltpu.make_async_remote_copy(
            src_ref=part_send.at[n],
            dst_ref=part_recv.at[turn],
            send_sem=part_send_sems.at[n],
            recv_sem=part_recv_sems.at[turn],
            device_id=core_at(a, layer, c),
            device_id_type=MESH,
        )

        @pl.when(turn != 0)
        def _():
            copy.start()

        @pl.when(turn == 0)
        def _():
            own_part[...] = part

        part_copies.append((turn, copy))

    total = own_part[...]
    for t in range(1, groups):
        pltpu.make_async_remote_copy(
            src_ref=part_send.at[0],
            dst_ref=part_recv.at[t],
            send_sem=part_send_sems.at[0],
            recv_sem=part_recv_sems.at[t],
            device_id=core_at(a, bit_xor(z, t, groups), c),
            device_id_type=MESH,
        ).wait_recv()
        total = total + part_recv[t].astype(F32)

    mixed = (total * count ** (-0.5)).astype(BF16).astype(F32)
    scaled = unit_channels(mixed, mid_gain[...].reshape(1, width)).astype(BF16)
    result = jnp.dot(scaled, out_weight[...], preferred_element_type=F32) * gate[...]
    out_ref[...] = result.reshape(cols, rows, width).astype(BF16)

    left_copy.wait_send()
    for copy in right_copies:
        copy.wait_send()
    for turn, copy in part_copies:

        @pl.when(turn != 0)
        def _(copy=copy):
            copy.wait_send()


def by_kernel(pair_state, in_gain, left_weight, right_weight, mid_gain, out_weight, out_gate):
    rows, cols, width = pair_state.shape
    groups = lax.axis_size("first")
    count = cols * lax.axis_size("second")
    pairs = rows * cols
    half = pairs // CORES
    changed = pl.pallas_call(
        functools.partial(triangle_kernel, groups, count),
        out_shape=jax.ShapeDtypeStruct((cols, rows, width), BF16),
        in_specs=[pl.BlockSpec(memory_space=pltpu.MemorySpace.HBM)] * 7,
        out_specs=pl.BlockSpec(memory_space=pltpu.VMEM),
        scratch_shapes=[
            pltpu.VMEM((cols, rows, width), BF16),
            pltpu.VMEM((width,), F32),
            pltpu.VMEM(left_weight.shape, BF16),
            pltpu.VMEM(right_weight.shape, BF16),
            pltpu.VMEM((width,), F32),
            pltpu.VMEM(out_weight.shape, BF16),
            pltpu.VMEM(out_gate.shape, BF16),
            pltpu.SemaphoreType.DMA((7,)),
            pltpu.VMEM((pairs, width), BF16),
            pltpu.VMEM((pairs, width), BF16),
            pltpu.VMEM((CORES, half, width), BF16),
            pltpu.VMEM((groups, CORES, half, width), BF16),
            pltpu.VMEM((pairs, width), F32),
            pltpu.VMEM((CORES, pairs, width), F32),
            pltpu.VMEM((CORES, half, width), F32),
            pltpu.VMEM((groups, pairs, width), BF16),
            pltpu.VMEM((groups, pairs, width), BF16),
            pltpu.VMEM((pairs, width), F32),
            pltpu.VMEM((pairs, width), F32),
            pltpu.SemaphoreType.DMA((2,)),
            pltpu.SemaphoreType.DMA((groups, CORES)),
            pltpu.SemaphoreType.DMA((groups, CORES)),
            pltpu.SemaphoreType.DMA((groups,)),
            pltpu.SemaphoreType.DMA((groups,)),
        ],
        compiler_params=pltpu.CompilerParams(
            collective_id=0, has_side_effects=True, vmem_limit_bytes=8 * 1024 * 1024
        ),
    )(
        *(
            pltpu.with_memory_space_constraint(value, pltpu.MemorySpace.HBM)
            for value in (
                jnp.swapaxes(pair_state, 0, 1),
                in_gain, left_weight, right_weight, mid_gain, out_weight, out_gate,
            )
        )
    )
    return jnp.swapaxes(changed, 0, 1)


def make_factors(pair_in, in_gain, left_weight, right_weight):
    ready = unit_channels(pair_in.astype(jnp.float32), in_gain).astype(jnp.bfloat16)
    ready = lax.optimization_barrier(ready)
    left = jnp.einsum("ijc,cd->ijd", ready, left_weight, preferred_element_type=jnp.float32)
    right = jnp.einsum("ijc,cd->ijd", ready, right_weight, preferred_element_type=jnp.float32)
    return (ready, left.astype(jnp.bfloat16), right.astype(jnp.bfloat16))


def finish_pair(mixed, ready, mid_gain, out_weight, out_gate):
    scaled = unit_channels(mixed.astype(jnp.float32), mid_gain).astype(jnp.bfloat16)
    scaled = lax.optimization_barrier(scaled)
    gate = jax.nn.sigmoid(
        jnp.einsum("ijc,cd->ijd", ready, out_gate, preferred_element_type=jnp.float32)
    )
    return (
        jnp.einsum("ijd,dc->ijc", scaled, out_weight, preferred_element_type=jnp.float32) * gate
    ).astype(jnp.bfloat16)


def by_collectives(pair_state, in_gain, left_weight, right_weight, mid_gain, out_weight, out_gate):
    ready, left, right = make_factors(pair_state, in_gain, left_weight, right_weight)
    count = pair_state.shape[1] * lax.axis_size("second")
    left_lines, right_lines = (
        lax.all_to_all(left, "second", split_axis=2, concat_axis=1, tiled=True),
        lax.all_to_all(right, "second", split_axis=2, concat_axis=1, tiled=True),
    )

    def meet(piece):
        return jnp.einsum("ikd,jkd->ijd", left_lines, piece, preferred_element_type=jnp.float32)

    strip = meet(lax.all_gather(right_lines, "first", axis=0, tiled=True))
    strip = (strip * count ** (-0.5)).astype(jnp.bfloat16)
    mixed = lax.all_to_all(strip, "second", split_axis=1, concat_axis=2, tiled=True)
    return finish_pair(mixed, ready, mid_gain, out_weight, out_gate)


def per_device(pair_state, *rest):
    groups, parts = lax.axis_size("first"), lax.axis_size("second")
    rows, cols, width = pair_state.shape
    fits = (
        parts == CORES * groups
        and groups > 1
        and groups & (groups - 1) == 0
        and rows == CORES * cols
        and rows % 8 == 0
        and rows * cols % 32 == 0
        and rows // 8 * cols <= 48
    )
    return (by_kernel if fits else by_collectives)(pair_state, *rest)


def solution(mesh):
    in_specs = (P("first", "second", None), P(), P(), P(), P(), P(), P())
    out_specs = P("first", "second", None)
    return jax.shard_map(
        per_device, mesh=mesh, in_specs=in_specs, out_specs=out_specs, check_vma=False
    )
```

```python
import functools

import jax
import jax.numpy as jnp
from jax import lax
from jax.experimental import pallas as pl
from jax.experimental.pallas import tpu as pltpu
from jax.sharding import PartitionSpec as P

MESH = pl.DeviceIdType.MESH
F32 = jnp.float32
BF16 = jnp.bfloat16
CORES = 2
PIECES = 2


def unit_channels(values, channel_gain):
    centred = values - jnp.mean(values, axis=-1, keepdims=True)
    return (
        centred
        * lax.rsqrt(jnp.mean(centred * centred, axis=-1, keepdims=True) + 1e-05)
        * channel_gain
    )


def bit_xor(left, right, count):
    total, bit = 0, 1
    while bit < count:
        total = total + (left // bit % 2 + right // bit % 2) % 2 * bit
        bit *= 2
    return total


def triangle_kernel(
    groups, count, pieces,
    x_hbm, in_gain_hbm, left_weight_hbm, right_weight_hbm, mid_gain_hbm, out_weight_hbm,
    out_gate_hbm, out_ref,
    x_ref, in_gain, left_weight, right_weight, mid_gain, out_weight, out_gate, fetch_sems,
    left_send, left_recv, right_send, right_recv, right_rows, left_f, right_f,
    part_send, part_recv, own_part, gate,
    left_sems, right_send_sems, right_recv_sems, part_send_sems, part_recv_sems,
):
    cols, rows, width = x_ref.shape
    half = rows // CORES
    some = half // pieces
    pairs = rows * cols
    a = lax.axis_index("first")
    b = lax.axis_index("second")
    z, c = b // CORES, b % CORES
    other = 1 - c

    def core_at(first, layer, core):
        return {"first": first, "second": layer * CORES + core}

    barrier = pltpu.get_barrier_semaphore()
    peers = [core_at(a, z, other)]
    for s in range(1, groups):
        peers += [core_at(bit_xor(a, s, groups), z, c), core_at(bit_xor(a, s, groups), z, other)]
        peers.append(core_at(a, bit_xor(z, s, groups), c))
    for peer in peers:
        pl.semaphore_signal(barrier, inc=1, device_id=peer, device_id_type=MESH)

    fetches = [
        pltpu.make_async_copy(src, dst, fetch_sems.at[n])
        for n, (src, dst) in enumerate([
            (x_hbm, x_ref), (in_gain_hbm, in_gain), (right_weight_hbm, right_weight),
            (left_weight_hbm, left_weight), (out_gate_hbm, out_gate),
            (mid_gain_hbm, mid_gain), (out_weight_hbm, out_weight),
        ])
    ]
    for fetch in fetches:
        fetch.start()
    got_x, got_in_gain, got_right, got_left, got_gate, got_mid_gain, got_out = fetches

    got_x.wait()
    got_in_gain.wait()
    values = x_ref[...].astype(F32).reshape(pairs, width)
    ready = unit_channels(values, in_gain[...].reshape(1, width)).astype(BF16)

    got_right.wait()
    right_rows[...] = jnp.dot(ready, right_weight[...], preferred_element_type=F32)
    for p in range(CORES):
        for h in range(pieces):
            for k in range(cols):
                start = k * rows + p * half + h * some
                right_f[p, k * some : (k + 1) * some, :] = right_rows[start : start + some, :]
            right_send[p, h] = right_f[p].astype(BF16)

    pl.semaphore_wait(barrier, len(peers))

    def right_copy(s, h, r):
        core = c if r == 0 else other
        return pltpu.make_async_remote_copy(
            src_ref=right_send.at[core, h],
            dst_ref=right_recv.at[s, h, r],
            send_sem=right_send_sems.at[s, h, r],
            recv_sem=right_recv_sems.at[s, h, r],
            device_id=core_at(bit_xor(a, s, groups), z, core),
            device_id_type=MESH,
        )

    order = [(0, h) for h in range(pieces)]
    order += [(s, h) for h in range(pieces) for s in range(groups // 2, groups)]
    order += [(s, h) for h in range(pieces) for s in range(1, groups // 2)]

    right_copies = []
    for s, h in order:
        for r in range(CORES):
            if s > 0 or r > 0:
                copy = right_copy(s, h, r)
                copy.start()
                right_copies.append(copy)

    got_left.wait()
    left = jnp.dot(ready, left_weight[...], preferred_element_type=F32).astype(BF16)
    left_send[...] = left
    left_f[0] = left.astype(F32)
    left_copy = pltpu.make_async_remote_copy(
        src_ref=left_send,
        dst_ref=left_recv,
        send_sem=left_sems.at[0],
        recv_sem=left_sems.at[1],
        device_id=core_at(a, z, other),
        device_id_type=MESH,
    )
    left_copy.start()

    got_gate.wait()
    gate[...] = jax.nn.sigmoid(jnp.dot(ready, out_gate[...], preferred_element_type=F32))

    left_copy.wait_recv()
    left_f[1] = left_recv[...].astype(F32)

    part_copies = []
    for s, h in order:
        if s == 0:
            right_f[0] = right_send[c, h].astype(F32)
        else:
            right_copy(s, h, 0).wait_recv()
            right_f[0] = right_recv[s, h, 0].astype(F32)
        right_copy(s, h, 1).wait_recv()
        right_f[1] = right_recv[s, h, 1].astype(F32)

        def step(k, sums):
            sums = list(sums)
            for r in range(CORES):
                line = left_f[r, pl.ds(pl.multiple_of(k * rows, 8), rows), :]
                for j in range(some):
                    sums[j] = sums[j] + line * right_f[r, pl.ds(k * some + j, 1), :]
            return tuple(sums)

        sums = lax.fori_loop(
            0, cols, step, tuple(jnp.zeros((rows, width), F32) for _ in range(some))
        )
        part = jnp.concatenate(sums, axis=0)
        part_send[s, h] = part.astype(BF16)
        layer = bit_xor(a, s, groups)
        turn = bit_xor(layer, z, groups)
        copy = pltpu.make_async_remote_copy(
            src_ref=part_send.at[s, h],
            dst_ref=part_recv.at[turn, h],
            send_sem=part_send_sems.at[s, h],
            recv_sem=part_recv_sems.at[turn, h],
            device_id=core_at(a, layer, c),
            device_id_type=MESH,
        )

        @pl.when(turn != 0)
        def _():
            copy.start()

        @pl.when(turn == 0)
        def _():
            own_part[h] = part

        part_copies.append((turn, copy))

    got_mid_gain.wait()
    got_out.wait()
    for h in range(pieces):
        total = own_part[h]
        for t in range(1, groups):
            pltpu.make_async_remote_copy(
                src_ref=part_send.at[0, h],
                dst_ref=part_recv.at[t, h],
                send_sem=part_send_sems.at[0, h],
                recv_sem=part_recv_sems.at[t, h],
                device_id=core_at(a, bit_xor(z, t, groups), c),
                device_id_type=MESH,
            ).wait_recv()
            total = total + part_recv[t, h].astype(F32)

        mixed = (total * count ** (-0.5)).astype(BF16).astype(F32)
        scaled = unit_channels(mixed, mid_gain[...].reshape(1, width)).astype(BF16)
        result = jnp.dot(scaled, out_weight[...], preferred_element_type=F32)
        result = result * gate[h * some * rows : (h + 1) * some * rows, :]
        out_ref[h * some : (h + 1) * some] = result.reshape(some, rows, width).astype(BF16)

    left_copy.wait_send()
    for copy in right_copies:
        copy.wait_send()
    for turn, copy in part_copies:

        @pl.when(turn != 0)
        def _(copy=copy):
            copy.wait_send()


def by_kernel(pair_state, in_gain, left_weight, right_weight, mid_gain, out_weight, out_gate):
    rows, cols, width = pair_state.shape
    groups = lax.axis_size("first")
    count = cols * lax.axis_size("second")
    pairs = rows * cols
    pieces = PIECES if rows // CORES % PIECES == 0 else 1
    some = rows // CORES // pieces
    changed = pl.pallas_call(
        functools.partial(triangle_kernel, groups, count, pieces),
        out_shape=jax.ShapeDtypeStruct((cols, rows, width), BF16),
        in_specs=[pl.BlockSpec(memory_space=pltpu.MemorySpace.HBM)] * 7,
        out_specs=pl.BlockSpec(memory_space=pltpu.VMEM),
        scratch_shapes=[
            pltpu.VMEM((cols, rows, width), BF16),
            pltpu.VMEM((width,), F32),
            pltpu.VMEM(left_weight.shape, BF16),
            pltpu.VMEM(right_weight.shape, BF16),
            pltpu.VMEM((width,), F32),
            pltpu.VMEM(out_weight.shape, BF16),
            pltpu.VMEM(out_gate.shape, BF16),
            pltpu.SemaphoreType.DMA((7,)),
            pltpu.VMEM((pairs, width), BF16),
            pltpu.VMEM((pairs, width), BF16),
            pltpu.VMEM((CORES, pieces, cols * some, width), BF16),
            pltpu.VMEM((groups, pieces, CORES, cols * some, width), BF16),
            pltpu.VMEM((pairs, width), F32),
            pltpu.VMEM((CORES, pairs, width), F32),
            pltpu.VMEM((CORES, cols * some, width), F32),
            pltpu.VMEM((groups, pieces, rows * some, width), BF16),
            pltpu.VMEM((groups, pieces, rows * some, width), BF16),
            pltpu.VMEM((pieces, rows * some, width), F32),
            pltpu.VMEM((pairs, width), F32),
            pltpu.SemaphoreType.DMA((2,)),
            pltpu.SemaphoreType.DMA((groups, pieces, CORES)),
            pltpu.SemaphoreType.DMA((groups, pieces, CORES)),
            pltpu.SemaphoreType.DMA((groups, pieces)),
            pltpu.SemaphoreType.DMA((groups, pieces)),
        ],
        compiler_params=pltpu.CompilerParams(
            collective_id=0, has_side_effects=True, vmem_limit_bytes=8 * 1024 * 1024
        ),
    )(
        *(
            pltpu.with_memory_space_constraint(value, pltpu.MemorySpace.HBM)
            for value in (
                jnp.swapaxes(pair_state, 0, 1),
                in_gain, left_weight, right_weight, mid_gain, out_weight, out_gate,
            )
        )
    )
    return jnp.swapaxes(changed, 0, 1)


def make_factors(pair_in, in_gain, left_weight, right_weight):
    ready = unit_channels(pair_in.astype(jnp.float32), in_gain).astype(jnp.bfloat16)
    ready = lax.optimization_barrier(ready)
    left = jnp.einsum("ijc,cd->ijd", ready, left_weight, preferred_element_type=jnp.float32)
    right = jnp.einsum("ijc,cd->ijd", ready, right_weight, preferred_element_type=jnp.float32)
    return (ready, left.astype(jnp.bfloat16), right.astype(jnp.bfloat16))


def finish_pair(mixed, ready, mid_gain, out_weight, out_gate):
    scaled = unit_channels(mixed.astype(jnp.float32), mid_gain).astype(jnp.bfloat16)
    scaled = lax.optimization_barrier(scaled)
    gate = jax.nn.sigmoid(
        jnp.einsum("ijc,cd->ijd", ready, out_gate, preferred_element_type=jnp.float32)
    )
    return (
        jnp.einsum("ijd,dc->ijc", scaled, out_weight, preferred_element_type=jnp.float32) * gate
    ).astype(jnp.bfloat16)


def by_collectives(pair_state, in_gain, left_weight, right_weight, mid_gain, out_weight, out_gate):
    ready, left, right = make_factors(pair_state, in_gain, left_weight, right_weight)
    count = pair_state.shape[1] * lax.axis_size("second")
    left_lines, right_lines = (
        lax.all_to_all(left, "second", split_axis=2, concat_axis=1, tiled=True),
        lax.all_to_all(right, "second", split_axis=2, concat_axis=1, tiled=True),
    )

    def meet(piece):
        return jnp.einsum("ikd,jkd->ijd", left_lines, piece, preferred_element_type=jnp.float32)

    strip = meet(lax.all_gather(right_lines, "first", axis=0, tiled=True))
    strip = (strip * count ** (-0.5)).astype(jnp.bfloat16)
    mixed = lax.all_to_all(strip, "second", split_axis=1, concat_axis=2, tiled=True)
    return finish_pair(mixed, ready, mid_gain, out_weight, out_gate)


def per_device(pair_state, *rest):
    groups, parts = lax.axis_size("first"), lax.axis_size("second")
    rows, cols, width = pair_state.shape
    fits = (
        parts == CORES * groups
        and groups > 1
        and groups & (groups - 1) == 0
        and rows == CORES * cols
        and rows % 8 == 0
        and rows * cols % 32 == 0
        and rows // 8 * cols <= 48
    )
    return (by_kernel if fits else by_collectives)(pair_state, *rest)


def solution(mesh):
    in_specs = (P("first", "second", None), P(), P(), P(), P(), P(), P())
    out_specs = P("first", "second", None)
    return jax.shard_map(
        per_device, mesh=mesh, in_specs=in_specs, out_specs=out_specs, check_vma=False
    )
```

```python
import functools

import jax
import jax.numpy as jnp
from jax import lax
from jax.experimental import pallas as pl
from jax.experimental.pallas import tpu as pltpu
from jax.sharding import PartitionSpec as P

MESH = pl.DeviceIdType.MESH
F32 = jnp.float32
BF16 = jnp.bfloat16
CORES = 2
PIECES = 2


def unit_channels(values, channel_gain):
    centred = values - jnp.mean(values, axis=-1, keepdims=True)
    return (
        centred
        * lax.rsqrt(jnp.mean(centred * centred, axis=-1, keepdims=True) + 1e-05)
        * channel_gain
    )


def bit_xor(left, right, count):
    total, bit = 0, 1
    while bit < count:
        total = total + (left // bit % 2 + right // bit % 2) % 2 * bit
        bit *= 2
    return total


def triangle_kernel(
    groups, count, pieces,
    x_hbm, in_gain_hbm, left_weight_hbm, right_weight_hbm, mid_gain_hbm, out_weight_hbm,
    out_gate_hbm, out_ref,
    x_ref, in_gain, left_weight, right_weight, mid_gain, out_weight, out_gate, fetch_sems,
    left_send, left_recv, right_send, right_recv, right_rows, left_f, right_f,
    part_send, part_recv, own_part, gate,
    line_sems, left_sems, right_send_sems, right_recv_sems, part_send_sems, part_recv_sems,
):
    cols, rows, width = x_ref.shape
    half = rows // CORES
    some = half // pieces
    pairs = rows * cols
    a = lax.axis_index("first")
    b = lax.axis_index("second")
    z, c = b // CORES, b % CORES
    other = 1 - c

    def core_at(first, layer, core):
        return {"first": first, "second": layer * CORES + core}

    barrier = pltpu.get_barrier_semaphore()
    peers = [core_at(a, z, other)]
    for s in range(1, groups):
        peers += [core_at(bit_xor(a, s, groups), z, c), core_at(bit_xor(a, s, groups), z, other)]
    for peer in peers:
        pl.semaphore_signal(barrier, inc=1, device_id=peer, device_id_type=MESH)

    def greet_line(semaphore):
        for there, near in ((z > 0, z - 1), (z < groups - 1, z + 1)):

            @pl.when(there)
            def _(near=near):
                pl.semaphore_signal(
                    semaphore, inc=1, device_id=core_at(a, near, c), device_id_type=MESH
                )

    neighbours = (z + groups - 1) // groups + (2 * groups - 2 - z) // groups
    greet_line(barrier)

    fetches = [
        pltpu.make_async_copy(src, dst, fetch_sems.at[n])
        for n, (src, dst) in enumerate([
            (x_hbm, x_ref), (in_gain_hbm, in_gain), (right_weight_hbm, right_weight),
            (left_weight_hbm, left_weight), (out_gate_hbm, out_gate),
            (mid_gain_hbm, mid_gain), (out_weight_hbm, out_weight),
        ])
    ]
    for fetch in fetches:
        fetch.start()
    got_x, got_in_gain, got_right, got_left, got_gate, got_mid_gain, got_out = fetches

    got_x.wait()
    got_in_gain.wait()
    values = x_ref[...].astype(F32).reshape(pairs, width)
    ready = unit_channels(values, in_gain[...].reshape(1, width)).astype(BF16)

    got_right.wait()
    right_rows[...] = jnp.dot(ready, right_weight[...], preferred_element_type=F32)
    for p in range(CORES):
        for h in range(pieces):
            for k in range(cols):
                start = k * rows + p * half + h * some
                right_f[p, k * some : (k + 1) * some, :] = right_rows[start : start + some, :]
            right_send[p, h] = right_f[p].astype(BF16)

    pl.semaphore_wait(barrier, len(peers) + neighbours)
    greet_line(line_sems.at[0])

    def right_copy(s, h, r):
        core = c if r == 0 else other
        return pltpu.make_async_remote_copy(
            src_ref=right_send.at[core, h],
            dst_ref=right_recv.at[s, h, r],
            send_sem=right_send_sems.at[s, h, r],
            recv_sem=right_recv_sems.at[s, h, r],
            device_id=core_at(bit_xor(a, s, groups), z, core),
            device_id_type=MESH,
        )

    order = [(0, h) for h in range(pieces)]
    order += [(s, h) for h in range(pieces) for s in range(groups // 2, groups)]
    order += [(s, h) for h in range(pieces) for s in range(1, groups // 2)]

    right_copies = []
    for s, h in order:
        for r in range(CORES):
            if s > 0 or r > 0:
                copy = right_copy(s, h, r)
                copy.start()
                right_copies.append(copy)

    got_left.wait()
    left = jnp.dot(ready, left_weight[...], preferred_element_type=F32).astype(BF16)
    left_send[...] = left
    left_f[0] = left.astype(F32)
    left_copy = pltpu.make_async_remote_copy(
        src_ref=left_send,
        dst_ref=left_recv,
        send_sem=left_sems.at[0],
        recv_sem=left_sems.at[1],
        device_id=core_at(a, z, other),
        device_id_type=MESH,
    )
    left_copy.start()

    got_gate.wait()
    gate[...] = jax.nn.sigmoid(jnp.dot(ready, out_gate[...], preferred_element_type=F32))

    for n in range(groups - 2):
        pl.semaphore_wait(line_sems.at[n], neighbours)
        if n + 1 < groups - 2:
            greet_line(line_sems.at[n + 1])

    left_copy.wait_recv()
    left_f[1] = left_recv[...].astype(F32)

    part_copies = []
    for s, h in order:
        if s == 0:
            right_f[0] = right_send[c, h].astype(F32)
        else:
            right_copy(s, h, 0).wait_recv()
            right_f[0] = right_recv[s, h, 0].astype(F32)
        right_copy(s, h, 1).wait_recv()
        right_f[1] = right_recv[s, h, 1].astype(F32)

        def step(k, sums):
            sums = list(sums)
            for r in range(CORES):
                line = left_f[r, pl.ds(pl.multiple_of(k * rows, 8), rows), :]
                for j in range(some):
                    sums[j] = sums[j] + line * right_f[r, pl.ds(k * some + j, 1), :]
            return tuple(sums)

        sums = lax.fori_loop(
            0, cols, step, tuple(jnp.zeros((rows, width), F32) for _ in range(some))
        )
        part = jnp.concatenate(sums, axis=0)
        part_send[s, h] = part.astype(BF16)
        layer = bit_xor(a, s, groups)
        turn = bit_xor(layer, z, groups)
        copy = pltpu.make_async_remote_copy(
            src_ref=part_send.at[s, h],
            dst_ref=part_recv.at[turn, h],
            send_sem=part_send_sems.at[s, h],
            recv_sem=part_recv_sems.at[turn, h],
            device_id=core_at(a, layer, c),
            device_id_type=MESH,
        )

        @pl.when(turn != 0)
        def _():
            copy.start()

        @pl.when(turn == 0)
        def _():
            own_part[h] = part

        part_copies.append((turn, copy))

    got_mid_gain.wait()
    got_out.wait()
    for h in range(pieces):
        total = own_part[h]
        for t in range(1, groups):
            pltpu.make_async_remote_copy(
                src_ref=part_send.at[0, h],
                dst_ref=part_recv.at[t, h],
                send_sem=part_send_sems.at[0, h],
                recv_sem=part_recv_sems.at[t, h],
                device_id=core_at(a, bit_xor(z, t, groups), c),
                device_id_type=MESH,
            ).wait_recv()
            total = total + part_recv[t, h].astype(F32)

        mixed = (total * count ** (-0.5)).astype(BF16).astype(F32)
        scaled = unit_channels(mixed, mid_gain[...].reshape(1, width)).astype(BF16)
        result = jnp.dot(scaled, out_weight[...], preferred_element_type=F32)
        result = result * gate[h * some * rows : (h + 1) * some * rows, :]
        out_ref[h * some : (h + 1) * some] = result.reshape(some, rows, width).astype(BF16)

    left_copy.wait_send()
    for copy in right_copies:
        copy.wait_send()
    for turn, copy in part_copies:

        @pl.when(turn != 0)
        def _(copy=copy):
            copy.wait_send()


def by_kernel(pair_state, in_gain, left_weight, right_weight, mid_gain, out_weight, out_gate):
    rows, cols, width = pair_state.shape
    groups = lax.axis_size("first")
    count = cols * lax.axis_size("second")
    pairs = rows * cols
    pieces = PIECES if rows // CORES % PIECES == 0 else 1
    some = rows // CORES // pieces
    changed = pl.pallas_call(
        functools.partial(triangle_kernel, groups, count, pieces),
        out_shape=jax.ShapeDtypeStruct((cols, rows, width), BF16),
        in_specs=[pl.BlockSpec(memory_space=pltpu.MemorySpace.HBM)] * 7,
        out_specs=pl.BlockSpec(memory_space=pltpu.VMEM),
        scratch_shapes=[
            pltpu.VMEM((cols, rows, width), BF16),
            pltpu.VMEM((width,), F32),
            pltpu.VMEM(left_weight.shape, BF16),
            pltpu.VMEM(right_weight.shape, BF16),
            pltpu.VMEM((width,), F32),
            pltpu.VMEM(out_weight.shape, BF16),
            pltpu.VMEM(out_gate.shape, BF16),
            pltpu.SemaphoreType.DMA((7,)),
            pltpu.VMEM((pairs, width), BF16),
            pltpu.VMEM((pairs, width), BF16),
            pltpu.VMEM((CORES, pieces, cols * some, width), BF16),
            pltpu.VMEM((groups, pieces, CORES, cols * some, width), BF16),
            pltpu.VMEM((pairs, width), F32),
            pltpu.VMEM((CORES, pairs, width), F32),
            pltpu.VMEM((CORES, cols * some, width), F32),
            pltpu.VMEM((groups, pieces, rows * some, width), BF16),
            pltpu.VMEM((groups, pieces, rows * some, width), BF16),
            pltpu.VMEM((pieces, rows * some, width), F32),
            pltpu.VMEM((pairs, width), F32),
            pltpu.SemaphoreType.REGULAR((groups - 2,)),
            pltpu.SemaphoreType.DMA((2,)),
            pltpu.SemaphoreType.DMA((groups, pieces, CORES)),
            pltpu.SemaphoreType.DMA((groups, pieces, CORES)),
            pltpu.SemaphoreType.DMA((groups, pieces)),
            pltpu.SemaphoreType.DMA((groups, pieces)),
        ],
        compiler_params=pltpu.CompilerParams(
            collective_id=0, has_side_effects=True, vmem_limit_bytes=8 * 1024 * 1024
        ),
    )(
        *(
            pltpu.with_memory_space_constraint(value, pltpu.MemorySpace.HBM)
            for value in (
                jnp.swapaxes(pair_state, 0, 1),
                in_gain, left_weight, right_weight, mid_gain, out_weight, out_gate,
            )
        )
    )
    return jnp.swapaxes(changed, 0, 1)


def make_factors(pair_in, in_gain, left_weight, right_weight):
    ready = unit_channels(pair_in.astype(jnp.float32), in_gain).astype(jnp.bfloat16)
    ready = lax.optimization_barrier(ready)
    left = jnp.einsum("ijc,cd->ijd", ready, left_weight, preferred_element_type=jnp.float32)
    right = jnp.einsum("ijc,cd->ijd", ready, right_weight, preferred_element_type=jnp.float32)
    return (ready, left.astype(jnp.bfloat16), right.astype(jnp.bfloat16))


def finish_pair(mixed, ready, mid_gain, out_weight, out_gate):
    scaled = unit_channels(mixed.astype(jnp.float32), mid_gain).astype(jnp.bfloat16)
    scaled = lax.optimization_barrier(scaled)
    gate = jax.nn.sigmoid(
        jnp.einsum("ijc,cd->ijd", ready, out_gate, preferred_element_type=jnp.float32)
    )
    return (
        jnp.einsum("ijd,dc->ijc", scaled, out_weight, preferred_element_type=jnp.float32) * gate
    ).astype(jnp.bfloat16)


def by_collectives(pair_state, in_gain, left_weight, right_weight, mid_gain, out_weight, out_gate):
    ready, left, right = make_factors(pair_state, in_gain, left_weight, right_weight)
    count = pair_state.shape[1] * lax.axis_size("second")
    left_lines, right_lines = (
        lax.all_to_all(left, "second", split_axis=2, concat_axis=1, tiled=True),
        lax.all_to_all(right, "second", split_axis=2, concat_axis=1, tiled=True),
    )

    def meet(piece):
        return jnp.einsum("ikd,jkd->ijd", left_lines, piece, preferred_element_type=jnp.float32)

    strip = meet(lax.all_gather(right_lines, "first", axis=0, tiled=True))
    strip = (strip * count ** (-0.5)).astype(jnp.bfloat16)
    mixed = lax.all_to_all(strip, "second", split_axis=1, concat_axis=2, tiled=True)
    return finish_pair(mixed, ready, mid_gain, out_weight, out_gate)


def per_device(pair_state, *rest):
    groups, parts = lax.axis_size("first"), lax.axis_size("second")
    rows, cols, width = pair_state.shape
    fits = (
        parts == CORES * groups
        and groups > 2
        and groups & (groups - 1) == 0
        and rows == CORES * cols
        and rows % 8 == 0
        and rows * cols % 32 == 0
        and rows // 8 * cols <= 48
    )
    return (by_kernel if fits else by_collectives)(pair_state, *rest)


def solution(mesh):
    in_specs = (P("first", "second", None), P(), P(), P(), P(), P(), P())
    out_specs = P("first", "second", None)
    return jax.shard_map(
        per_device, mesh=mesh, in_specs=in_specs, out_specs=out_specs, check_vma=False
    )
```

```python
import functools

import jax
import jax.numpy as jnp
from jax import lax
from jax.experimental import pallas as pl
from jax.experimental.pallas import tpu as pltpu
from jax.sharding import PartitionSpec as P

MESH = pl.DeviceIdType.MESH
F32 = jnp.float32
BF16 = jnp.bfloat16
CORES = 2
PIECES = 2


def unit_channels(values, channel_gain):
    centred = values - jnp.mean(values, axis=-1, keepdims=True)
    return (
        centred
        * lax.rsqrt(jnp.mean(centred * centred, axis=-1, keepdims=True) + 1e-05)
        * channel_gain
    )


def bit_xor(left, right, count):
    total, bit = 0, 1
    while bit < count:
        total = total + (left // bit % 2 + right // bit % 2) % 2 * bit
        bit *= 2
    return total


def triangle_kernel(
    groups, count, pieces,
    x_hbm, in_gain_hbm, left_weight_hbm, right_weight_hbm, mid_gain_hbm, out_weight_hbm,
    out_gate_hbm, out_ref,
    x_ref, in_gain, left_weight, right_weight, mid_gain, out_weight, out_gate, fetch_sems,
    left_send, left_recv, right_send, right_recv, right_rows, left_f, right_f,
    part_send, part_recv, own_part, gate,
    line_sems, left_sems, right_send_sems, right_recv_sems, part_send_sems, part_recv_sems,
):
    cols, rows, width = x_ref.shape
    half = rows // CORES
    some = half // pieces
    pairs = rows * cols
    a = lax.axis_index("first")
    b = lax.axis_index("second")
    z, c = b // CORES, b % CORES
    other = 1 - c

    def core_at(first, layer, core):
        return {"first": first, "second": layer * CORES + core}

    barrier = pltpu.get_barrier_semaphore()
    peers = [core_at(a, z, other)]
    for s in range(1, groups):
        peers += [core_at(bit_xor(a, s, groups), z, c), core_at(bit_xor(a, s, groups), z, other)]
    for peer in peers:
        pl.semaphore_signal(barrier, inc=1, device_id=peer, device_id_type=MESH)

    def greet_line(semaphore):
        for there, near in ((z > 0, z - 1), (z < groups - 1, z + 1)):

            @pl.when(there)
            def _(near=near):
                pl.semaphore_signal(
                    semaphore, inc=1, device_id=core_at(a, near, c), device_id_type=MESH
                )

    neighbours = (z + groups - 1) // groups + (2 * groups - 2 - z) // groups
    greet_line(barrier)

    fetches = [
        pltpu.make_async_copy(src, dst, fetch_sems.at[n])
        for n, (src, dst) in enumerate([
            (x_hbm, x_ref), (in_gain_hbm, in_gain), (right_weight_hbm, right_weight),
            (left_weight_hbm, left_weight), (out_gate_hbm, out_gate),
            (mid_gain_hbm, mid_gain), (out_weight_hbm, out_weight),
        ])
    ]
    for fetch in fetches:
        fetch.start()
    got_x, got_in_gain, got_right, got_left, got_gate, got_mid_gain, got_out = fetches

    got_x.wait()
    got_in_gain.wait()
    values = x_ref[...].astype(F32).reshape(pairs, width)
    ready = unit_channels(values, in_gain[...].reshape(1, width)).astype(BF16)

    got_right.wait()
    right_rows[...] = jnp.dot(ready, right_weight[...], preferred_element_type=F32)
    for p in range(CORES):
        for h in range(pieces):
            for k in range(cols):
                start = k * rows + p * half + h * some
                right_f[p, k * some : (k + 1) * some, :] = right_rows[start : start + some, :]
            right_send[p, h] = right_f[p].astype(BF16)

    pl.semaphore_wait(barrier, len(peers) + neighbours)
    greet_line(line_sems.at[0])

    def right_copy(s, h, r):
        core = c if r == 0 else other
        return pltpu.make_async_remote_copy(
            src_ref=right_send.at[core, h],
            dst_ref=right_recv.at[s, h, r],
            send_sem=right_send_sems.at[s, h, r],
            recv_sem=right_recv_sems.at[s, h, r],
            device_id=core_at(bit_xor(a, s, groups), z, core),
            device_id_type=MESH,
        )

    order = [(s, h) for s in (0, groups - 1) for h in range(pieces)]
    order += [(s, h) for h in range(pieces) for s in range(groups - 2, 0, -1)]

    right_copies = []
    for s, h in order:
        for r in range(CORES):
            if s > 0 or r > 0:
                copy = right_copy(s, h, r)
                copy.start()
                right_copies.append(copy)

    got_left.wait()
    left = jnp.dot(ready, left_weight[...], preferred_element_type=F32).astype(BF16)
    left_send[...] = left
    left_f[0] = left.astype(F32)
    left_copy = pltpu.make_async_remote_copy(
        src_ref=left_send,
        dst_ref=left_recv,
        send_sem=left_sems.at[0],
        recv_sem=left_sems.at[1],
        device_id=core_at(a, z, other),
        device_id_type=MESH,
    )
    left_copy.start()

    got_gate.wait()
    gate[...] = jax.nn.sigmoid(jnp.dot(ready, out_gate[...], preferred_element_type=F32))

    for n in range(groups - 2):
        pl.semaphore_wait(line_sems.at[n], neighbours)
        if n + 1 < groups - 2:
            greet_line(line_sems.at[n + 1])

    left_copy.wait_recv()
    left_f[1] = left_recv[...].astype(F32)

    part_copies = []
    for s, h in order:
        if s == 0:
            right_f[0] = right_send[c, h].astype(F32)
        else:
            right_copy(s, h, 0).wait_recv()
            right_f[0] = right_recv[s, h, 0].astype(F32)
        right_copy(s, h, 1).wait_recv()
        right_f[1] = right_recv[s, h, 1].astype(F32)

        def step(k, sums):
            sums = list(sums)
            for r in range(CORES):
                line = left_f[r, pl.ds(pl.multiple_of(k * rows, 8), rows), :]
                for j in range(some):
                    sums[j] = sums[j] + line * right_f[r, pl.ds(k * some + j, 1), :]
            return tuple(sums)

        sums = lax.fori_loop(
            0, cols, step, tuple(jnp.zeros((rows, width), F32) for _ in range(some))
        )
        part = jnp.concatenate(sums, axis=0)
        part_send[s, h] = part.astype(BF16)
        layer = bit_xor(a, s, groups)
        turn = bit_xor(layer, z, groups)
        copy = pltpu.make_async_remote_copy(
            src_ref=part_send.at[s, h],
            dst_ref=part_recv.at[turn, h],
            send_sem=part_send_sems.at[s, h],
            recv_sem=part_recv_sems.at[turn, h],
            device_id=core_at(a, layer, c),
            device_id_type=MESH,
        )

        @pl.when(turn != 0)
        def _():
            copy.start()

        @pl.when(turn == 0)
        def _():
            own_part[h] = part

        part_copies.append((turn, copy))

    got_mid_gain.wait()
    got_out.wait()
    for h in range(pieces):
        total = own_part[h]
        for t in range(1, groups):
            pltpu.make_async_remote_copy(
                src_ref=part_send.at[0, h],
                dst_ref=part_recv.at[t, h],
                send_sem=part_send_sems.at[0, h],
                recv_sem=part_recv_sems.at[t, h],
                device_id=core_at(a, bit_xor(z, t, groups), c),
                device_id_type=MESH,
            ).wait_recv()
            total = total + part_recv[t, h].astype(F32)

        mixed = (total * count ** (-0.5)).astype(BF16).astype(F32)
        scaled = unit_channels(mixed, mid_gain[...].reshape(1, width)).astype(BF16)
        result = jnp.dot(scaled, out_weight[...], preferred_element_type=F32)
        result = result * gate[h * some * rows : (h + 1) * some * rows, :]
        out_ref[h * some : (h + 1) * some] = result.reshape(some, rows, width).astype(BF16)

    left_copy.wait_send()
    for copy in right_copies:
        copy.wait_send()
    for turn, copy in part_copies:

        @pl.when(turn != 0)
        def _(copy=copy):
            copy.wait_send()


def by_kernel(pair_state, in_gain, left_weight, right_weight, mid_gain, out_weight, out_gate):
    rows, cols, width = pair_state.shape
    groups = lax.axis_size("first")
    count = cols * lax.axis_size("second")
    pairs = rows * cols
    pieces = PIECES if rows // CORES % PIECES == 0 else 1
    some = rows // CORES // pieces
    changed = pl.pallas_call(
        functools.partial(triangle_kernel, groups, count, pieces),
        out_shape=jax.ShapeDtypeStruct((cols, rows, width), BF16),
        in_specs=[pl.BlockSpec(memory_space=pltpu.MemorySpace.HBM)] * 7,
        out_specs=pl.BlockSpec(memory_space=pltpu.VMEM),
        scratch_shapes=[
            pltpu.VMEM((cols, rows, width), BF16),
            pltpu.VMEM((width,), F32),
            pltpu.VMEM(left_weight.shape, BF16),
            pltpu.VMEM(right_weight.shape, BF16),
            pltpu.VMEM((width,), F32),
            pltpu.VMEM(out_weight.shape, BF16),
            pltpu.VMEM(out_gate.shape, BF16),
            pltpu.SemaphoreType.DMA((7,)),
            pltpu.VMEM((pairs, width), BF16),
            pltpu.VMEM((pairs, width), BF16),
            pltpu.VMEM((CORES, pieces, cols * some, width), BF16),
            pltpu.VMEM((groups, pieces, CORES, cols * some, width), BF16),
            pltpu.VMEM((pairs, width), F32),
            pltpu.VMEM((CORES, pairs, width), F32),
            pltpu.VMEM((CORES, cols * some, width), F32),
            pltpu.VMEM((groups, pieces, rows * some, width), BF16),
            pltpu.VMEM((groups, pieces, rows * some, width), BF16),
            pltpu.VMEM((pieces, rows * some, width), F32),
            pltpu.VMEM((pairs, width), F32),
            pltpu.SemaphoreType.REGULAR((groups - 2,)),
            pltpu.SemaphoreType.DMA((2,)),
            pltpu.SemaphoreType.DMA((groups, pieces, CORES)),
            pltpu.SemaphoreType.DMA((groups, pieces, CORES)),
            pltpu.SemaphoreType.DMA((groups, pieces)),
            pltpu.SemaphoreType.DMA((groups, pieces)),
        ],
        compiler_params=pltpu.CompilerParams(
            collective_id=0, has_side_effects=True, vmem_limit_bytes=8 * 1024 * 1024
        ),
    )(
        *(
            pltpu.with_memory_space_constraint(value, pltpu.MemorySpace.HBM)
            for value in (
                jnp.swapaxes(pair_state, 0, 1),
                in_gain, left_weight, right_weight, mid_gain, out_weight, out_gate,
            )
        )
    )
    return jnp.swapaxes(changed, 0, 1)


def make_factors(pair_in, in_gain, left_weight, right_weight):
    ready = unit_channels(pair_in.astype(jnp.float32), in_gain).astype(jnp.bfloat16)
    ready = lax.optimization_barrier(ready)
    left = jnp.einsum("ijc,cd->ijd", ready, left_weight, preferred_element_type=jnp.float32)
    right = jnp.einsum("ijc,cd->ijd", ready, right_weight, preferred_element_type=jnp.float32)
    return (ready, left.astype(jnp.bfloat16), right.astype(jnp.bfloat16))


def finish_pair(mixed, ready, mid_gain, out_weight, out_gate):
    scaled = unit_channels(mixed.astype(jnp.float32), mid_gain).astype(jnp.bfloat16)
    scaled = lax.optimization_barrier(scaled)
    gate = jax.nn.sigmoid(
        jnp.einsum("ijc,cd->ijd", ready, out_gate, preferred_element_type=jnp.float32)
    )
    return (
        jnp.einsum("ijd,dc->ijc", scaled, out_weight, preferred_element_type=jnp.float32) * gate
    ).astype(jnp.bfloat16)


def by_collectives(pair_state, in_gain, left_weight, right_weight, mid_gain, out_weight, out_gate):
    ready, left, right = make_factors(pair_state, in_gain, left_weight, right_weight)
    count = pair_state.shape[1] * lax.axis_size("second")
    left_lines, right_lines = (
        lax.all_to_all(left, "second", split_axis=2, concat_axis=1, tiled=True),
        lax.all_to_all(right, "second", split_axis=2, concat_axis=1, tiled=True),
    )

    def meet(piece):
        return jnp.einsum("ikd,jkd->ijd", left_lines, piece, preferred_element_type=jnp.float32)

    strip = meet(lax.all_gather(right_lines, "first", axis=0, tiled=True))
    strip = (strip * count ** (-0.5)).astype(jnp.bfloat16)
    mixed = lax.all_to_all(strip, "second", split_axis=1, concat_axis=2, tiled=True)
    return finish_pair(mixed, ready, mid_gain, out_weight, out_gate)


def per_device(pair_state, *rest):
    groups, parts = lax.axis_size("first"), lax.axis_size("second")
    rows, cols, width = pair_state.shape
    fits = (
        parts == CORES * groups
        and groups > 2
        and groups & (groups - 1) == 0
        and rows == CORES * cols
        and rows % 8 == 0
        and rows * cols % 32 == 0
        and rows // 8 * cols <= 48
    )
    return (by_kernel if fits else by_collectives)(pair_state, *rest)


def solution(mesh):
    in_specs = (P("first", "second", None), P(), P(), P(), P(), P(), P())
    out_specs = P("first", "second", None)
    return jax.shard_map(
        per_device, mesh=mesh, in_specs=in_specs, out_specs=out_specs, check_vma=False
    )
```

```python
import functools

import jax
import jax.numpy as jnp
from jax import lax
from jax.experimental import pallas as pl
from jax.experimental.pallas import tpu as pltpu
from jax.sharding import PartitionSpec as P

MESH = pl.DeviceIdType.MESH
F32 = jnp.float32
BF16 = jnp.bfloat16
CORES = 2
PIECES = 2


def unit_channels(values, channel_gain):
    centred = values - jnp.mean(values, axis=-1, keepdims=True)
    return (
        centred
        * lax.rsqrt(jnp.mean(centred * centred, axis=-1, keepdims=True) + 1e-05)
        * channel_gain
    )


def bit_xor(left, right, count):
    total, bit = 0, 1
    while bit < count:
        total = total + (left // bit % 2 + right // bit % 2) % 2 * bit
        bit *= 2
    return total


def triangle_kernel(
    groups, count, pieces,
    x_hbm, in_gain_hbm, left_weight_hbm, right_weight_hbm, mid_gain_hbm, out_weight_hbm,
    out_gate_hbm, out_ref,
    x_ref, in_gain, left_weight, right_weight, mid_gain, out_weight, out_gate, fetch_sems,
    left_send, left_recv, right_send, right_recv, right_rows, left_f, right_f,
    part_send, part_recv, own_part, gate,
    left_sems, right_send_sems, right_recv_sems, part_send_sems, part_recv_sems,
):
    cols, rows, width = x_ref.shape
    half = rows // CORES
    some = half // pieces
    pairs = rows * cols
    a = lax.axis_index("first")
    b = lax.axis_index("second")
    z, c = b // CORES, b % CORES
    other = 1 - c

    def core_at(first, layer, core):
        return {"first": first, "second": layer * CORES + core}

    barrier = pltpu.get_barrier_semaphore()
    peers = [core_at(a, z, other)]
    for s in range(1, groups):
        peers += [core_at(bit_xor(a, s, groups), z, c), core_at(bit_xor(a, s, groups), z, other)]
        peers.append(core_at(a, bit_xor(z, s, groups), c))
    for peer in peers:
        pl.semaphore_signal(barrier, inc=1, device_id=peer, device_id_type=MESH)

    fetches = [
        pltpu.make_async_copy(src, dst, fetch_sems.at[n])
        for n, (src, dst) in enumerate([
            (x_hbm, x_ref), (in_gain_hbm, in_gain), (right_weight_hbm, right_weight),
            (left_weight_hbm, left_weight), (out_gate_hbm, out_gate),
            (mid_gain_hbm, mid_gain), (out_weight_hbm, out_weight),
        ])
    ]
    for fetch in fetches:
        fetch.start()
    got_x, got_in_gain, got_right, got_left, got_gate, got_mid_gain, got_out = fetches

    got_x.wait()
    got_in_gain.wait()
    values = x_ref[...].astype(F32).reshape(pairs, width)
    ready = unit_channels(values, in_gain[...].reshape(1, width)).astype(BF16)

    got_right.wait()
    right_rows[...] = jnp.dot(ready, right_weight[...], preferred_element_type=F32)
    for p in range(CORES):
        for h in range(pieces):
            for k in range(cols):
                start = k * rows + p * half + h * some
                right_f[p, k * some : (k + 1) * some, :] = right_rows[start : start + some, :]
            right_send[p, h] = right_f[p].astype(BF16)

    pl.semaphore_wait(barrier, len(peers))

    def right_copy(s, h, r):
        core = c if r == 0 else other
        return pltpu.make_async_remote_copy(
            src_ref=right_send.at[core, h],
            dst_ref=right_recv.at[s, h, r],
            send_sem=right_send_sems.at[s, h, r],
            recv_sem=right_recv_sems.at[s, h, r],
            device_id=core_at(bit_xor(a, s, groups), z, core),
            device_id_type=MESH,
        )

    order = [(s, h) for s in (0, groups - 1) for h in range(pieces)]
    order += [(s, h) for h in range(pieces) for s in range(groups - 2, 0, -1)]

    right_copies = []
    for s, h in order:
        for r in range(CORES):
            if s > 0 or r > 0:
                copy = right_copy(s, h, r)
                copy.start()
                right_copies.append(copy)

    got_left.wait()
    left = jnp.dot(ready, left_weight[...], preferred_element_type=F32).astype(BF16)
    left_send[...] = left
    left_f[0] = left.astype(F32)
    left_copy = pltpu.make_async_remote_copy(
        src_ref=left_send,
        dst_ref=left_recv,
        send_sem=left_sems.at[0],
        recv_sem=left_sems.at[1],
        device_id=core_at(a, z, other),
        device_id_type=MESH,
    )
    left_copy.start()

    got_gate.wait()
    gate[...] = jax.nn.sigmoid(jnp.dot(ready, out_gate[...], preferred_element_type=F32))

    left_copy.wait_recv()
    left_f[1] = left_recv[...].astype(F32)

    part_copies = []
    for s, h in order:
        if s == 0:
            right_f[0] = right_send[c, h].astype(F32)
        else:
            right_copy(s, h, 0).wait_recv()
            right_f[0] = right_recv[s, h, 0].astype(F32)
        right_copy(s, h, 1).wait_recv()
        right_f[1] = right_recv[s, h, 1].astype(F32)

        def step(k, sums):
            sums = list(sums)
            for r in range(CORES):
                line = left_f[r, pl.ds(pl.multiple_of(k * rows, 8), rows), :]
                for j in range(some):
                    sums[j] = sums[j] + line * right_f[r, pl.ds(k * some + j, 1), :]
            return tuple(sums)

        sums = lax.fori_loop(
            0, cols, step, tuple(jnp.zeros((rows, width), F32) for _ in range(some))
        )
        part = jnp.concatenate(sums, axis=0)
        part_send[s, h] = part.astype(BF16)
        layer = bit_xor(a, s, groups)
        turn = bit_xor(layer, z, groups)
        copy = pltpu.make_async_remote_copy(
            src_ref=part_send.at[s, h],
            dst_ref=part_recv.at[turn, h],
            send_sem=part_send_sems.at[s, h],
            recv_sem=part_recv_sems.at[turn, h],
            device_id=core_at(a, layer, c),
            device_id_type=MESH,
        )

        @pl.when(turn != 0)
        def _():
            copy.start()

        @pl.when(turn == 0)
        def _():
            own_part[h] = part

        part_copies.append((turn, copy))

    got_mid_gain.wait()
    got_out.wait()
    for h in range(pieces):
        total = own_part[h]
        for t in range(1, groups):
            pltpu.make_async_remote_copy(
                src_ref=part_send.at[0, h],
                dst_ref=part_recv.at[t, h],
                send_sem=part_send_sems.at[0, h],
                recv_sem=part_recv_sems.at[t, h],
                device_id=core_at(a, bit_xor(z, t, groups), c),
                device_id_type=MESH,
            ).wait_recv()
            total = total + part_recv[t, h].astype(F32)

        mixed = (total * count ** (-0.5)).astype(BF16).astype(F32)
        scaled = unit_channels(mixed, mid_gain[...].reshape(1, width)).astype(BF16)
        result = jnp.dot(scaled, out_weight[...], preferred_element_type=F32)
        result = result * gate[h * some * rows : (h + 1) * some * rows, :]
        out_ref[h * some : (h + 1) * some] = result.reshape(some, rows, width).astype(BF16)

    left_copy.wait_send()
    for copy in right_copies:
        copy.wait_send()
    for turn, copy in part_copies:

        @pl.when(turn != 0)
        def _(copy=copy):
            copy.wait_send()


def by_kernel(pair_state, in_gain, left_weight, right_weight, mid_gain, out_weight, out_gate):
    rows, cols, width = pair_state.shape
    groups = lax.axis_size("first")
    count = cols * lax.axis_size("second")
    pairs = rows * cols
    pieces = PIECES if rows // CORES % PIECES == 0 else 1
    some = rows // CORES // pieces
    changed = pl.pallas_call(
        functools.partial(triangle_kernel, groups, count, pieces),
        out_shape=jax.ShapeDtypeStruct((cols, rows, width), BF16),
        in_specs=[pl.BlockSpec(memory_space=pltpu.MemorySpace.HBM)] * 7,
        out_specs=pl.BlockSpec(memory_space=pltpu.VMEM),
        scratch_shapes=[
            pltpu.VMEM((cols, rows, width), BF16),
            pltpu.VMEM((width,), F32),
            pltpu.VMEM(left_weight.shape, BF16),
            pltpu.VMEM(right_weight.shape, BF16),
            pltpu.VMEM((width,), F32),
            pltpu.VMEM(out_weight.shape, BF16),
            pltpu.VMEM(out_gate.shape, BF16),
            pltpu.SemaphoreType.DMA((7,)),
            pltpu.VMEM((pairs, width), BF16),
            pltpu.VMEM((pairs, width), BF16),
            pltpu.VMEM((CORES, pieces, cols * some, width), BF16),
            pltpu.VMEM((groups, pieces, CORES, cols * some, width), BF16),
            pltpu.VMEM((pairs, width), F32),
            pltpu.VMEM((CORES, pairs, width), F32),
            pltpu.VMEM((CORES, cols * some, width), F32),
            pltpu.VMEM((groups, pieces, rows * some, width), BF16),
            pltpu.VMEM((groups, pieces, rows * some, width), BF16),
            pltpu.VMEM((pieces, rows * some, width), F32),
            pltpu.VMEM((pairs, width), F32),
            pltpu.SemaphoreType.DMA((2,)),
            pltpu.SemaphoreType.DMA((groups, pieces, CORES)),
            pltpu.SemaphoreType.DMA((groups, pieces, CORES)),
            pltpu.SemaphoreType.DMA((groups, pieces)),
            pltpu.SemaphoreType.DMA((groups, pieces)),
        ],
        compiler_params=pltpu.CompilerParams(
            collective_id=0, has_side_effects=True, vmem_limit_bytes=8 * 1024 * 1024
        ),
    )(
        *(
            pltpu.with_memory_space_constraint(value, pltpu.MemorySpace.HBM)
            for value in (
                jnp.swapaxes(pair_state, 0, 1),
                in_gain, left_weight, right_weight, mid_gain, out_weight, out_gate,
            )
        )
    )
    return jnp.swapaxes(changed, 0, 1)


def make_factors(pair_in, in_gain, left_weight, right_weight):
    ready = unit_channels(pair_in.astype(jnp.float32), in_gain).astype(jnp.bfloat16)
    ready = lax.optimization_barrier(ready)
    left = jnp.einsum("ijc,cd->ijd", ready, left_weight, preferred_element_type=jnp.float32)
    right = jnp.einsum("ijc,cd->ijd", ready, right_weight, preferred_element_type=jnp.float32)
    return (ready, left.astype(jnp.bfloat16), right.astype(jnp.bfloat16))


def finish_pair(mixed, ready, mid_gain, out_weight, out_gate):
    scaled = unit_channels(mixed.astype(jnp.float32), mid_gain).astype(jnp.bfloat16)
    scaled = lax.optimization_barrier(scaled)
    gate = jax.nn.sigmoid(
        jnp.einsum("ijc,cd->ijd", ready, out_gate, preferred_element_type=jnp.float32)
    )
    return (
        jnp.einsum("ijd,dc->ijc", scaled, out_weight, preferred_element_type=jnp.float32) * gate
    ).astype(jnp.bfloat16)


def by_collectives(pair_state, in_gain, left_weight, right_weight, mid_gain, out_weight, out_gate):
    ready, left, right = make_factors(pair_state, in_gain, left_weight, right_weight)
    count = pair_state.shape[1] * lax.axis_size("second")
    left_lines, right_lines = (
        lax.all_to_all(left, "second", split_axis=2, concat_axis=1, tiled=True),
        lax.all_to_all(right, "second", split_axis=2, concat_axis=1, tiled=True),
    )

    def meet(piece):
        return jnp.einsum("ikd,jkd->ijd", left_lines, piece, preferred_element_type=jnp.float32)

    strip = meet(lax.all_gather(right_lines, "first", axis=0, tiled=True))
    strip = (strip * count ** (-0.5)).astype(jnp.bfloat16)
    mixed = lax.all_to_all(strip, "second", split_axis=1, concat_axis=2, tiled=True)
    return finish_pair(mixed, ready, mid_gain, out_weight, out_gate)


def per_device(pair_state, *rest):
    groups, parts = lax.axis_size("first"), lax.axis_size("second")
    rows, cols, width = pair_state.shape
    fits = (
        parts == CORES * groups
        and groups > 1
        and groups & (groups - 1) == 0
        and rows == CORES * cols
        and rows % 8 == 0
        and rows * cols % 32 == 0
        and rows // 8 * cols <= 48
    )
    return (by_kernel if fits else by_collectives)(pair_state, *rest)


def solution(mesh):
    in_specs = (P("first", "second", None), P(), P(), P(), P(), P(), P())
    out_specs = P("first", "second", None)
    return jax.shard_map(
        per_device, mesh=mesh, in_specs=in_specs, out_specs=out_specs, check_vma=False
    )
```

```python
import functools

import jax
import jax.numpy as jnp
from jax import lax
from jax.experimental import pallas as pl
from jax.experimental.pallas import tpu as pltpu
from jax.sharding import PartitionSpec as P

MESH = pl.DeviceIdType.MESH
F32 = jnp.float32
BF16 = jnp.bfloat16
CORES = 2
PIECES = 2


def unit_channels(values, channel_gain):
    centred = values - jnp.mean(values, axis=-1, keepdims=True)
    return (
        centred
        * lax.rsqrt(jnp.mean(centred * centred, axis=-1, keepdims=True) + 1e-05)
        * channel_gain
    )


def bit_xor(left, right, count):
    total, bit = 0, 1
    while bit < count:
        total = total + (left // bit % 2 + right // bit % 2) % 2 * bit
        bit *= 2
    return total


def triangle_kernel(
    groups, count, pieces,
    x_hbm, in_gain_hbm, left_weight_hbm, right_weight_hbm, mid_gain_hbm, out_weight_hbm,
    out_gate_hbm, out_ref,
    x_ref, in_gain, left_weight, right_weight, mid_gain, out_weight, out_gate, fetch_sems,
    left_send, left_recv, right_send, right_recv, right_rows, left_f, right_f,
    part_send, part_recv, own_part, gate,
    left_sems, right_send_sems, right_recv_sems, part_send_sems, part_recv_sems,
):
    cols, rows, width = x_ref.shape
    half = rows // CORES
    some = half // pieces
    pairs = rows * cols
    a = lax.axis_index("first")
    b = lax.axis_index("second")
    z, c = b // CORES, b % CORES
    other = 1 - c

    def core_at(first, layer, core):
        return {"first": first, "second": layer * CORES + core}

    barrier = pltpu.get_barrier_semaphore()
    peers = [core_at(a, z, other)]
    for s in range(1, groups):
        peers += [core_at(bit_xor(a, s, groups), z, c), core_at(bit_xor(a, s, groups), z, other)]
        peers.append(core_at(a, bit_xor(z, s, groups), c))
    for peer in peers:
        pl.semaphore_signal(barrier, inc=1, device_id=peer, device_id_type=MESH)

    fetches = [
        pltpu.make_async_copy(src, dst, fetch_sems.at[n])
        for n, (src, dst) in enumerate([
            (x_hbm, x_ref), (in_gain_hbm, in_gain), (right_weight_hbm, right_weight),
            (left_weight_hbm, left_weight), (out_gate_hbm, out_gate),
            (mid_gain_hbm, mid_gain), (out_weight_hbm, out_weight),
        ])
    ]
    for fetch in fetches:
        fetch.start()
    got_x, got_in_gain, got_right, got_left, got_gate, got_mid_gain, got_out = fetches

    got_x.wait()
    got_in_gain.wait()
    values = x_ref[...].astype(F32).reshape(pairs, width)
    ready = unit_channels(values, in_gain[...].reshape(1, width)).astype(BF16)

    got_right.wait()
    right_rows[...] = jnp.dot(ready, right_weight[...], preferred_element_type=F32)
    for p in range(CORES):
        for h in range(pieces):
            for k in range(cols):
                start = k * rows + p * half + h * some
                right_f[p, k * some : (k + 1) * some, :] = right_rows[start : start + some, :]
            right_send[p, h] = right_f[p].astype(BF16)

    pl.semaphore_wait(barrier, len(peers))

    def right_copy(s, h, r):
        core = c if r == 0 else other
        return pltpu.make_async_remote_copy(
            src_ref=right_send.at[core, h],
            dst_ref=right_recv.at[s, h, r],
            send_sem=right_send_sems.at[s, h, r],
            recv_sem=right_recv_sems.at[s, h, r],
            device_id=core_at(bit_xor(a, s, groups), z, core),
            device_id_type=MESH,
        )

    order = [(s, h) for s in (0, groups - 1) for h in range(pieces)]
    order += [(s, h) for h in range(pieces) for s in range(groups - 2, 0, -1)]

    right_copies = []
    for s, h in order:
        for r in range(CORES):
            if s > 0 or r > 0:
                copy = right_copy(s, h, r)
                copy.start()
                right_copies.append(copy)

    got_left.wait()
    left = jnp.dot(ready, left_weight[...], preferred_element_type=F32).astype(BF16)
    left_send[...] = left
    left_f[0] = left.astype(F32)
    left_copy = pltpu.make_async_remote_copy(
        src_ref=left_send,
        dst_ref=left_recv,
        send_sem=left_sems.at[0],
        recv_sem=left_sems.at[1],
        device_id=core_at(a, z, other),
        device_id_type=MESH,
    )
    left_copy.start()

    left_copy.wait_recv()
    left_f[1] = left_recv[...].astype(F32)

    part_copies = []
    for s, h in order:
        if s == 0:
            right_f[0] = right_send[c, h].astype(F32)
        else:
            right_copy(s, h, 0).wait_recv()
            right_f[0] = right_recv[s, h, 0].astype(F32)
        right_copy(s, h, 1).wait_recv()
        right_f[1] = right_recv[s, h, 1].astype(F32)

        def step(k, sums):
            sums = list(sums)
            for r in range(CORES):
                line = left_f[r, pl.ds(pl.multiple_of(k * rows, 8), rows), :]
                for j in range(some):
                    sums[j] = sums[j] + line * right_f[r, pl.ds(k * some + j, 1), :]
            return tuple(sums)

        sums = lax.fori_loop(
            0, cols, step, tuple(jnp.zeros((rows, width), F32) for _ in range(some))
        )
        part = jnp.concatenate(sums, axis=0)
        part_send[s, h] = part.astype(BF16)
        layer = bit_xor(a, s, groups)
        turn = bit_xor(layer, z, groups)
        copy = pltpu.make_async_remote_copy(
            src_ref=part_send.at[s, h],
            dst_ref=part_recv.at[turn, h],
            send_sem=part_send_sems.at[s, h],
            recv_sem=part_recv_sems.at[turn, h],
            device_id=core_at(a, layer, c),
            device_id_type=MESH,
        )

        @pl.when(turn != 0)
        def _():
            copy.start()

        @pl.when(turn == 0)
        def _():
            own_part[h] = part

        part_copies.append((turn, copy))

    got_gate.wait()
    gate[...] = jax.nn.sigmoid(jnp.dot(ready, out_gate[...], preferred_element_type=F32))
    got_mid_gain.wait()
    got_out.wait()
    for h in range(pieces):
        total = own_part[h]
        for t in range(1, groups):
            pltpu.make_async_remote_copy(
                src_ref=part_send.at[0, h],
                dst_ref=part_recv.at[t, h],
                send_sem=part_send_sems.at[0, h],
                recv_sem=part_recv_sems.at[t, h],
                device_id=core_at(a, bit_xor(z, t, groups), c),
                device_id_type=MESH,
            ).wait_recv()
            total = total + part_recv[t, h].astype(F32)

        mixed = (total * count ** (-0.5)).astype(BF16).astype(F32)
        scaled = unit_channels(mixed, mid_gain[...].reshape(1, width)).astype(BF16)
        result = jnp.dot(scaled, out_weight[...], preferred_element_type=F32)
        result = result * gate[h * some * rows : (h + 1) * some * rows, :]
        out_ref[h * some : (h + 1) * some] = result.reshape(some, rows, width).astype(BF16)

    left_copy.wait_send()
    for copy in right_copies:
        copy.wait_send()
    for turn, copy in part_copies:

        @pl.when(turn != 0)
        def _(copy=copy):
            copy.wait_send()


def by_kernel(pair_state, in_gain, left_weight, right_weight, mid_gain, out_weight, out_gate):
    rows, cols, width = pair_state.shape
    groups = lax.axis_size("first")
    count = cols * lax.axis_size("second")
    pairs = rows * cols
    pieces = PIECES if rows // CORES % PIECES == 0 else 1
    some = rows // CORES // pieces
    changed = pl.pallas_call(
        functools.partial(triangle_kernel, groups, count, pieces),
        out_shape=jax.ShapeDtypeStruct((cols, rows, width), BF16),
        in_specs=[pl.BlockSpec(memory_space=pltpu.MemorySpace.HBM)] * 7,
        out_specs=pl.BlockSpec(memory_space=pltpu.VMEM),
        scratch_shapes=[
            pltpu.VMEM((cols, rows, width), BF16),
            pltpu.VMEM((width,), F32),
            pltpu.VMEM(left_weight.shape, BF16),
            pltpu.VMEM(right_weight.shape, BF16),
            pltpu.VMEM((width,), F32),
            pltpu.VMEM(out_weight.shape, BF16),
            pltpu.VMEM(out_gate.shape, BF16),
            pltpu.SemaphoreType.DMA((7,)),
            pltpu.VMEM((pairs, width), BF16),
            pltpu.VMEM((pairs, width), BF16),
            pltpu.VMEM((CORES, pieces, cols * some, width), BF16),
            pltpu.VMEM((groups, pieces, CORES, cols * some, width), BF16),
            pltpu.VMEM((pairs, width), F32),
            pltpu.VMEM((CORES, pairs, width), F32),
            pltpu.VMEM((CORES, cols * some, width), F32),
            pltpu.VMEM((groups, pieces, rows * some, width), BF16),
            pltpu.VMEM((groups, pieces, rows * some, width), BF16),
            pltpu.VMEM((pieces, rows * some, width), F32),
            pltpu.VMEM((pairs, width), F32),
            pltpu.SemaphoreType.DMA((2,)),
            pltpu.SemaphoreType.DMA((groups, pieces, CORES)),
            pltpu.SemaphoreType.DMA((groups, pieces, CORES)),
            pltpu.SemaphoreType.DMA((groups, pieces)),
            pltpu.SemaphoreType.DMA((groups, pieces)),
        ],
        compiler_params=pltpu.CompilerParams(
            collective_id=0, has_side_effects=True, vmem_limit_bytes=8 * 1024 * 1024
        ),
    )(
        *(
            pltpu.with_memory_space_constraint(value, pltpu.MemorySpace.HBM)
            for value in (
                jnp.swapaxes(pair_state, 0, 1),
                in_gain, left_weight, right_weight, mid_gain, out_weight, out_gate,
            )
        )
    )
    return jnp.swapaxes(changed, 0, 1)


def make_factors(pair_in, in_gain, left_weight, right_weight):
    ready = unit_channels(pair_in.astype(jnp.float32), in_gain).astype(jnp.bfloat16)
    ready = lax.optimization_barrier(ready)
    left = jnp.einsum("ijc,cd->ijd", ready, left_weight, preferred_element_type=jnp.float32)
    right = jnp.einsum("ijc,cd->ijd", ready, right_weight, preferred_element_type=jnp.float32)
    return (ready, left.astype(jnp.bfloat16), right.astype(jnp.bfloat16))


def finish_pair(mixed, ready, mid_gain, out_weight, out_gate):
    scaled = unit_channels(mixed.astype(jnp.float32), mid_gain).astype(jnp.bfloat16)
    scaled = lax.optimization_barrier(scaled)
    gate = jax.nn.sigmoid(
        jnp.einsum("ijc,cd->ijd", ready, out_gate, preferred_element_type=jnp.float32)
    )
    return (
        jnp.einsum("ijd,dc->ijc", scaled, out_weight, preferred_element_type=jnp.float32) * gate
    ).astype(jnp.bfloat16)


def by_collectives(pair_state, in_gain, left_weight, right_weight, mid_gain, out_weight, out_gate):
    ready, left, right = make_factors(pair_state, in_gain, left_weight, right_weight)
    count = pair_state.shape[1] * lax.axis_size("second")
    left_lines, right_lines = (
        lax.all_to_all(left, "second", split_axis=2, concat_axis=1, tiled=True),
        lax.all_to_all(right, "second", split_axis=2, concat_axis=1, tiled=True),
    )

    def meet(piece):
        return jnp.einsum("ikd,jkd->ijd", left_lines, piece, preferred_element_type=jnp.float32)

    strip = meet(lax.all_gather(right_lines, "first", axis=0, tiled=True))
    strip = (strip * count ** (-0.5)).astype(jnp.bfloat16)
    mixed = lax.all_to_all(strip, "second", split_axis=1, concat_axis=2, tiled=True)
    return finish_pair(mixed, ready, mid_gain, out_weight, out_gate)


def per_device(pair_state, *rest):
    groups, parts = lax.axis_size("first"), lax.axis_size("second")
    rows, cols, width = pair_state.shape
    fits = (
        parts == CORES * groups
        and groups > 1
        and groups & (groups - 1) == 0
        and rows == CORES * cols
        and rows % 8 == 0
        and rows * cols % 32 == 0
        and rows // 8 * cols <= 48
    )
    return (by_kernel if fits else by_collectives)(pair_state, *rest)


def solution(mesh):
    in_specs = (P("first", "second", None), P(), P(), P(), P(), P(), P())
    out_specs = P("first", "second", None)
    return jax.shard_map(
        per_device, mesh=mesh, in_specs=in_specs, out_specs=out_specs, check_vma=False
    )
```
